32 devices in a mesh: seq: 8 (over z, x), head: 4 (over y, core).
Axes of the slice: x: 2, y: 2, z: 4, core: 2. Of those that a mesh axis runs over, the one named last changes fastest.
Arguments:
- queries: bfloat16 [6144, 8192], P('seq', 'head'), may hold values from -6 to 6
- key_rows: bfloat16 [6144, 8192], P('seq', 'head'), may hold values from -0.5 to 0.5
- value_rows: bfloat16 [6144, 8192], P('seq', 'head'), may hold values from -130 to 130
- log_decay: float32 [64, 6144], P('head', 'seq'), may hold values from -1 to 0
- norm_gain: float32 [8192], P('head'), may hold values from 0.1 to 1.9
- grad_out: bfloat16 [6144, 8192], P('seq', 'head'), may hold values from -13 to 13
Outputs:
- output: bfloat16 [6144, 8192], P('seq', 'head')
- grad_queries: bfloat16 [6144, 8192], P('seq', 'head')
- grad_keys: bfloat16 [6144, 8192], P('seq', 'head')
- grad_values: bfloat16 [6144, 8192], P('seq', 'head')
- grad_gain: float32 [8192], P('head')
The draws below stay inside these ranges and needn't reach their ends.
All inputs are finite; a program needn't handle non-finite values.
Results may differ from the reference program's by a relative error of at most 0.01.
Values sent between devices are 32-bit elements; how exact they have to be, the bound alone decides.
A program may use at most 192 MiB of HBM per device.

```python
import jax
import jax.numpy as jnp
from jax import lax

HEADS = 64
DH = 128
TOK_DEV = 768
SEQUENCE_TOKENS = 6144
HD = 8192


def draw_log_decay(key, part):
    sample_sequences = jax.random.split(key, 6)
    token_position = jnp.arange(SEQUENCE_TOKENS)
    fast_share = 0.5
    picked = jax.random.uniform(sample_sequences[0], (HEADS, 1), dtype=jnp.float32)
    fast_rate = jnp.exp(jax.random.uniform(sample_sequences[1], (HEADS, 1), dtype=jnp.float32, minval=jnp.log(1.0 / 50.0), maxval=jnp.log(1.0 / 30.0)))
    slow_rate = 0.6 / SEQUENCE_TOKENS
    baseline_decay_rate = jnp.where(picked < fast_share, fast_rate, slow_rate)
    block_count = SEQUENCE_TOKENS // TOK_DEV
    block_multiplier = jnp.exp(jax.random.uniform(sample_sequences[2], (HEADS, block_count), dtype=jnp.float32, minval=jnp.log(0.5), maxval=jnp.log(2.0)))
    block_multiplier = jnp.repeat(block_multiplier, TOK_DEV, axis=1, total_repeat_length=SEQUENCE_TOKENS)
    jitter_amplitude = jax.random.uniform(sample_sequences[3], (HEADS, SEQUENCE_TOKENS), dtype=jnp.float32, minval=0.5, maxval=1.5)
    spike_locations = jax.random.randint(sample_sequences[4], (3,), 0, SEQUENCE_TOKENS)
    spike_magnitude = jax.random.uniform(sample_sequences[5], (HEADS, 3), dtype=jnp.float32, minval=0.22, maxval=0.69)
    decay_spikes = jnp.sum(jnp.where(token_position[None, :, None] == spike_locations[None, None, :], spike_magnitude[:, None, :], 0.0), axis=2)
    return (-(baseline_decay_rate * block_multiplier * jitter_amplitude + decay_spikes)).astype(jnp.float32)


def draw_value_rows(key, part):
    sample_sequences = jax.random.split(key, 3)
    head_number = (jnp.arange(HD) // DH).astype(jnp.float32)
    head_scale = 1.0 + 2.0 * head_number / max(HEADS - 1, 1)
    base = jnp.clip(jax.random.normal(sample_sequences[0], (SEQUENCE_TOKENS, HD), dtype=jnp.float32), -4.0, 4.0)
    row_scale = jnp.exp(jax.random.uniform(sample_sequences[2], (SEQUENCE_TOKENS, 1), dtype=jnp.float32, minval=0.0, maxval=jnp.log(10.0)))
    return (base * head_scale[None, :] * row_scale).astype(jnp.bfloat16)


def draw_grad_out(key, part):
    sample_sequences = jax.random.split(key, 1)
    ramp = 1.0 + 2.0 * jnp.arange(SEQUENCE_TOKENS).astype(jnp.float32) / (SEQUENCE_TOKENS - 1)
    base = jnp.clip(jax.random.normal(sample_sequences[0], (SEQUENCE_TOKENS, HD), dtype=jnp.float32), -4.0, 4.0)
    return (base * ramp[:, None]).astype(jnp.bfloat16)


def level_of(rng, dims, cuts, least, largest):
    def one(axis_at, parts):
        draws = jax.random.uniform(jax.random.fold_in(jax.random.fold_in(rng, 6), axis_at), (parts,), jnp.float32, least / len(cuts), largest / len(cuts))
        return jnp.repeat(jnp.exp(draws), dims[axis_at] // parts).reshape((-1,) + (1,) * (len(dims) - axis_at - 1))

    factor_of = one(*cuts[0])
    for cut in cuts[1:]:
        factor_of = factor_of * one(*cut)
    return factor_of


def normal_values(rng, extent, width, limit, cuts=(), held_as=jnp.bfloat16):
    result = jax.random.normal(rng, extent, jnp.float32) * width
    if len(cuts) > 0:
        result = level_of(rng, extent, cuts, -0.22, 0.18) * result
    return jnp.clip(result, min=-limit, max=limit).astype(held_as)


def setup_inputs(seed: int = 0) -> dict:
    arg_keys = jax.random.split(jax.random.key(seed), 7)
    queries = normal_values(arg_keys[0], (SEQUENCE_TOKENS, HD), 1.0, 6.0, ((0, 8), (1, 4)))
    key_rows = normal_values(arg_keys[1], (SEQUENCE_TOKENS, HD), DH ** -0.5, 0.5, ((0, 8), (1, 4)))
    value_rows = draw_value_rows(jax.random.fold_in(arg_keys[6], 71), 0)
    log_decay = draw_log_decay(jax.random.fold_in(arg_keys[6], 71), 0)
    norm_gain = jnp.clip(1.0 + 0.18 * jax.random.normal(arg_keys[4], (HD,), jnp.float32), 0.1, 1.9)
    grad_out = draw_grad_out(jax.random.fold_in(arg_keys[6], 71), 0)
    return dict(queries=queries, key_rows=key_rows, value_rows=value_rows, log_decay=log_decay, norm_gain=norm_gain, grad_out=grad_out)


EPSILON = 1e-06

def exact_product(form, left, right):
    return jnp.einsum(form, left.astype(jnp.float32), right.astype(jnp.float32), precision=lax.Precision.HIGHEST)

def plain_product(form, left, right):
    return jnp.einsum(form, left.astype(jnp.float32), right.astype(jnp.float32))

def causal_decay(cumulative):
    length = cumulative.shape[-1]
    below_diag = jnp.arange(length)[:, None] >= jnp.arange(length)[None, :]
    spread = cumulative[..., :, None] - cumulative[..., None, :]
    return jnp.where(below_diag, jnp.exp(jnp.where(below_diag, spread, 0.0)), 0.0)

def split_heads(matrix):
    return matrix.reshape(matrix.shape[0], HEADS, DH).transpose(1, 0, 2)

def merge_heads(tensor):
    return tensor.transpose(1, 0, 2).reshape(tensor.shape[1], HD)

def attend(q_heads, k_heads, v_heads, cumulative, state):
    decay_mask = causal_decay(cumulative)
    scores = plain_product('htd,hsd->hts', q_heads, k_heads)
    weights = (scores * decay_mask).astype(jnp.bfloat16)
    attended = plain_product('hts,hsd->htd', weights, v_heads)
    attended = attended + jnp.exp(cumulative)[..., None] * exact_product('htd,hde->hte', q_heads, state)
    return (attended, weights, decay_mask)

def normalize(attended, grad_rows, norm_gain):
    mixed = merge_heads(attended)
    inverse = lax.rsqrt(lax.optimization_barrier(jnp.mean(mixed * mixed, axis=1)) + EPSILON)
    normed = mixed * inverse[:, None]
    scaled = grad_rows.astype(jnp.float32) * norm_gain[None, :]
    center = lax.optimization_barrier(jnp.mean(scaled * normed, axis=1))
    grad_attended = (inverse[:, None] * (scaled - normed * center[:, None])).astype(jnp.bfloat16)
    return (normed, split_heads(grad_attended))

def reference(queries, key_rows, value_rows, log_decay, norm_gain, grad_out):
    blocks = SEQUENCE_TOKENS // TOK_DEV

    def tile(matrix):
        return matrix.reshape(blocks, TOK_DEV, HEADS, DH).transpose(0, 2, 1, 3)
    q_all = tile(queries)
    k_all = tile(key_rows)
    v_all = tile(value_rows)
    grad_rows = grad_out.reshape(blocks, TOK_DEV, HD)
    cumulative = jnp.cumsum(log_decay.reshape(HEADS, blocks, TOK_DEV).transpose(1, 0, 2), axis=2)
    block_total = cumulative[:, :, -1]

    def local_fn(operands):
        k_heads, v_heads, cumul, last_value = operands
        tail = jnp.exp(last_value[:, None] - cumul)
        return exact_product('htd,hte->hde', k_heads.astype(jnp.float32) * tail[..., None], v_heads)
    local_state = lax.map(local_fn, (k_all, v_all, cumulative, block_total))

    def carry_step(carry, operands):
        decay_total, local_term = operands
        return (decay_total[:, None, None] * carry + local_term, carry)
    zero_state = jnp.zeros((HEADS, DH, DH), jnp.float32)
    _, state_in = lax.scan(carry_step, zero_state, (jnp.exp(block_total), local_state))

    def second_pass(operands):
        q_heads, k_heads, v_heads, grad_block, cumul, state = operands
        attended, _, _ = attend(q_heads, k_heads, v_heads, cumul, state)
        normed, grad_heads = normalize(attended, grad_block, norm_gain)
        output_block = (normed * norm_gain[None, :]).astype(jnp.bfloat16)
        gain_part = lax.optimization_barrier(jnp.sum(grad_block.astype(jnp.float32) * normed, axis=0))
        state_grad = exact_product('htd,hte->hde', q_heads.astype(jnp.float32) * jnp.exp(cumul)[..., None], grad_heads)
        return (output_block, gain_part, state_grad)
    output, gain_parts, state_grad = lax.map(second_pass, (q_all, k_all, v_all, grad_rows, cumulative, state_in))
    _, state_after = lax.scan(carry_step, zero_state, (jnp.exp(block_total), state_grad), reverse=True)

    def fourth_pass(operands):
        q_heads, k_heads, v_heads, grad_block, cumul, last_value, state, after = operands
        attended, weights, decay_mask = attend(q_heads, k_heads, v_heads, cumul, state)
        _, grad_heads = normalize(attended, grad_block, norm_gain)
        grad_weights = (plain_product('htd,hsd->hts', grad_heads, v_heads) * decay_mask).astype(jnp.bfloat16)
        tail = jnp.exp(last_value[:, None] - cumul)[..., None]
        grad_q = plain_product('hts,hsd->htd', grad_weights, k_heads)
        grad_q = grad_q + jnp.exp(cumul)[..., None] * exact_product('hte,hde->htd', grad_heads, state)
        grad_k = plain_product('hts,htd->hsd', grad_weights, q_heads)
        grad_k = grad_k + tail * exact_product('hse,hde->hsd', v_heads, after)
        grad_v = plain_product('hts,htd->hsd', weights, grad_heads)
        grad_v = grad_v + tail * exact_product('hsd,hde->hse', k_heads, after)
        return (merge_heads(grad_q).astype(jnp.bfloat16), merge_heads(grad_k).astype(jnp.bfloat16), merge_heads(grad_v).astype(jnp.bfloat16))
    grad_q, grad_k, grad_v = lax.map(fourth_pass, (q_all, k_all, v_all, grad_rows, cumulative, block_total, state_in, state_after))
    grad_gain = lax.optimization_barrier(jnp.sum(gain_parts, axis=0))
    return (output.reshape(SEQUENCE_TOKENS, HD), grad_q.reshape(SEQUENCE_TOKENS, HD), grad_k.reshape(SEQUENCE_TOKENS, HD), grad_v.reshape(SEQUENCE_TOKENS, HD), grad_gain)
```

```python
import functools

import jax
import jax.numpy as jnp
from jax import lax
from jax.experimental import pallas as pl
from jax.experimental.pallas import tpu as pltpu
from jax.sharding import PartitionSpec as P

DH = 128
EPSILON = 1e-06
CHUNK = 128
F32 = jnp.float32
BF16 = jnp.bfloat16
MESH = pl.DeviceIdType.MESH
HIGHEST = lax.Precision.HIGHEST

AB = ((1,), (0,))
ABT = ((1,), (1,))
ATB = ((0,), (0,))
E_MID, E_TOTAL, E_BEFORE, E_AFTER = range(4)


def mm(left, right, dims):
    return lax.dot_general(left, right, (dims, ((), ())), preferred_element_type=F32)


def exact(left, right, dims):
    return lax.dot_general(left, right, (dims, ((), ())), precision=HIGHEST, preferred_element_type=F32)


def remote(src, dst, send, recv, axis, target):
    return pltpu.make_async_remote_copy(
        src_ref=src, dst_ref=dst, send_sem=send, recv_sem=recv,
        device_id={axis: target}, device_id_type=MESH,
    )


def loop(count, body):
    lax.fori_loop(0, count, lambda i, c: (body(i), c)[1], 0)


def spans(tokens):
    return [slice(j * CHUNK, (j + 1) * CHUNK) for j in range(tokens // CHUNK)]


def causal(x):
    t = lax.broadcasted_iota(jnp.int32, x.shape, 0)
    s = lax.broadcasted_iota(jnp.int32, x.shape, 1)
    return jnp.where(t >= s, x, 0.0).astype(BF16)


def three_terms(x):
    high = x.astype(BF16).astype(F32)
    middle = (x - high).astype(BF16).astype(F32)
    return [high, middle, x - high - middle]


def decay_tables(ld_ref, columns, rows, whole):
    heads, tokens = ld_ref.shape
    below = lax.broadcasted_iota(jnp.int32, (CHUNK, CHUNK), 0)
    right = lax.broadcasted_iota(jnp.int32, (CHUNK, CHUNK), 1)
    tri = (below <= right).astype(F32)
    totals = []
    for j, span in enumerate(spans(tokens)):
        cum = exact(ld_ref[:, span], tri, AB)
        total = jnp.broadcast_to(cum[:, CHUNK - 1 : CHUNK], (heads, DH))
        middle = 0.5 * total
        parts = three_terms(jnp.exp(cum - middle)) + three_terms(jnp.exp(middle - cum))
        rest = columns.shape[1] - 6 * heads
        if rest:
            parts.append(jnp.zeros((rest, CHUNK), F32))
        columns[span] = jnp.concatenate(parts, axis=0).T.astype(BF16)
        rows[E_MID, j] = jnp.exp(middle)
        rows[E_TOTAL, j] = jnp.exp(total)
        totals.append(total)
    count = len(totals)
    run = jnp.zeros((heads, DH), F32)
    for j in range(count):
        rows[E_BEFORE, j] = jnp.exp(run + 0.5 * totals[j])
        run = run + totals[j]
    whole[...] = jnp.exp(run)
    run = jnp.zeros((heads, DH), F32)
    for j in reversed(range(count)):
        rows[E_AFTER, j] = jnp.exp(run + 0.5 * totals[j])
        run = run + totals[j]


def selector(columns, heads, h, first):
    r = lax.broadcasted_iota(jnp.int32, (columns.shape[1], DH), 0) - h - first * heads
    return jnp.where((r == 0) | (r == heads) | (r == 2 * heads), 1.0, 0.0).astype(BF16)


class Chain:
    def __init__(self, n, index, reverse, whole, partner_whole, bufs, recv_sems, send_sems):
        (self.lsend, self.lrecv, self.zsend, self.zrecv, self.xsend, self.xrecv) = bufs
        self.recv_sems, self.send_sems, self.index = recv_sems, send_sems, index
        self.whole, self.partner_whole = whole, partner_whole
        me = lax.axis_index("seq")
        self.partner = me + 1 - 2 * lax.rem(me, 2)
        place = n - 1 - me if reverse else me
        self.later = lax.rem(place, 2)
        self.row = place // 2
        self.first = self.row == 0
        self.last = self.row == n // 2 - 1
        step = -2 if reverse else 2
        self.next = lax.rem(me + step + n, n)

    def led(self, s):
        return 2 * s + 1 - self.later

    def other(self, s):
        return 2 * s + self.later

    def copy(self, kind, src, dst, h, target):
        return remote(src, dst, self.send_sems.at[self.index, kind], self.recv_sems.at[kind, h], "seq", target)

    def copy_l(self, h):
        return self.copy(0, self.lsend.at[h], self.lrecv.at[h], h, self.partner)

    def copy_x(self, h):
        return self.copy(1, self.xsend.at[h], self.xrecv.at[h], h, self.partner)

    def copy_z(self, h):
        return self.copy(2, self.zsend.at[h], self.zrecv.at[h], h, self.next)

    def start(self):
        @pl.when(self.first)
        def _():
            self.zrecv[...] = jnp.zeros_like(self.zrecv)

    def step(self, h, take):
        self.copy_l(h).wait_recv()

        @pl.when(jnp.logical_not(self.first))
        def _():
            self.copy_z(h).wait_recv()

        state = self.zrecv[h]
        own, theirs = self.whole[pl.ds(h, 1), :], self.partner_whole[pl.ds(h, 1), :]

        @pl.when(self.later == 1)
        def _():
            mid = theirs * state + self.lrecv[h]
            self.zsend[h] = own * mid + self.lsend[h]
            self.xsend[h] = state
            take(h, mid)

        @pl.when(self.later == 0)
        def _():
            mid = own * state + self.lsend[h]
            self.zsend[h] = theirs * mid + self.lrecv[h]
            self.xsend[h] = mid
            take(h, state)

        @pl.when(jnp.logical_not(self.last))
        def _():
            self.copy_z(h).start()

        self.copy_x(h).start()

    def take(self, h, take):
        self.copy_x(h).wait_recv()
        take(h, self.xrecv[h])

    def wait_l(self, half):
        self.copy(0, self.lsend.at[0:half], self.lrecv.at[0:half], 0, self.partner).wait_send()

    def wait_xz(self, half):
        self.copy(1, self.xsend.at[0:half], self.xrecv.at[0:half], 0, self.partner).wait_send()

        @pl.when(jnp.logical_not(self.last))
        def _():
            self.copy(2, self.zsend.at[0:half], self.zrecv.at[0:half], 0, self.next).wait_send()


def main_kernel(
    n, peers,
    q_hbm, k_hbm, v_hbm, g_hbm, ld_ref, gain_ref,
    q, k, kd, g, att, obuf, r_out, rows, gg_out,
    v, qd, ga, wt, qs, ts, columns, state_in, sq_acc, in_acc, inv_b, cen_b,
    whole, partner_whole,
    stat_send, stat_recv, gain_send, gain_recv,
    lsend, lrecv, zsend, zrecv, xsend, xrecv,
    load_sem, g_sem, recv_sems, send_sems, pair_sem, stat_sem, gain_sem,
):
    heads, tokens, _ = q.shape
    half = heads // 2
    parts = list(enumerate(spans(tokens)))
    final = len(parts) - 1
    me = lax.axis_index("seq")
    my_head = lax.axis_index("head")
    width = heads * DH * peers

    barrier = pltpu.get_barrier_semaphore()
    for off in range(1, n):
        pl.semaphore_signal(barrier, inc=1, device_id={"seq": lax.rem(me + off, n)}, device_id_type=MESH)
    for off in range(1, peers):
        pl.semaphore_signal(barrier, inc=1, device_id={"head": lax.rem(my_head + off, peers)}, device_id_type=MESH)

    def load(hbm, vmem, h, sem):
        where = pl.ds(pl.multiple_of(h * DH, DH), DH)
        pltpu.make_async_copy(hbm.at[:, where], vmem.at[h], sem).start()

    def landed(vmem, count, sem):
        pltpu.make_async_copy(vmem.at[0:count], vmem.at[0:count], sem).wait()

    def load_kv(p):
        for h in (2 * p, 2 * p + 1):
            load(k_hbm, k, h, load_sem.at[0, p])
            load(v_hbm, v, h, load_sem.at[0, p])

    def load_q(p):
        for h in (2 * p, 2 * p + 1):
            load(q_hbm, q, h, load_sem.at[1, p])

    def load_g(p):
        for h in (2 * p, 2 * p + 1):
            load(g_hbm, g, h, g_sem)

    loop(half, load_kv)
    loop(half, load_q)
    loop(half, load_g)
    decay_tables(ld_ref, columns, rows, whole)
    bufs = (lsend, lrecv, zsend, zrecv, xsend, xrecv)
    forward = Chain(n, 0, False, whole, partner_whole, bufs, recv_sems, send_sems)
    backward = Chain(n, 1, True, whole, partner_whole, bufs, recv_sems, send_sems)
    forward.start()

    def row(kind, j, h):
        return rows[kind, j, pl.ds(h, 1), :]

    def local_pair(p):
        landed(k, 4, load_sem.at[0, p])
        keys = {}
        for i, h in enumerate((2 * p, 2 * p + 1)):
            pick = selector(columns, heads, h, 3)
            for j, span in parts:
                keys[i, j] = (k[h, span].astype(F32) * mm(columns[span], pick, AB)).astype(BF16)
                kd[h, span] = keys[i, j]
        for i, h in enumerate((2 * p, 2 * p + 1)):
            state = None
            for j, span in parts:
                part = row(E_MID, j, h) * mm(keys[i, j], v[h, span], ATB)
                if j:
                    qs[h, j] = (row(E_MID, j, h) * state).astype(BF16)
                state = part if j == 0 else row(E_TOTAL, j, h) * state + part
            lsend[h] = state

    def pair_copy():
        return remote(whole, partner_whole, pair_sem.at[0], pair_sem.at[1], "seq", forward.partner)

    local_pair(0)
    pl.semaphore_wait(barrier, n - 1 + peers - 1)
    pair_copy().start()
    forward.copy_l(forward.other(0)).start()

    def local_rest(i):
        local_pair(i + 1)
        forward.copy_l(forward.other(i + 1)).start()

    loop(half - 1, local_rest)

    def intra_pair(p):
        landed(q, 2, load_sem.at[1, p])
        queries, weights = {}, {}
        both = [(i, j, 2 * p + i, span) for i in (0, 1) for j, span in parts]
        picks = [selector(columns, heads, 2 * p + i, 0) for i in (0, 1)]
        for i, j, h, span in both:
            queries[i, j] = (q[h, span].astype(F32) * mm(columns[span], picks[i], AB)).astype(BF16)
            qd[h, span] = queries[i, j]
        for i, j, h, span in both:
            weights[i, j] = causal(mm(queries[i, j], kd[h, span], ABT))
            wt[h, span] = weights[i, j].T
        for i, j, h, span in both:
            if j:
                left = jnp.concatenate([weights[i, j], queries[i, j]], axis=1)
                right = jnp.concatenate([v[h, span], qs[h, j]], axis=0)
                att[h, span] = mm(left, right, AB)
            else:
                att[h, span] = mm(weights[i, j], v[h, span], AB)

    def arrive(h):
        state = state_in[h].astype(BF16)
        gain = gain_ref[pl.ds(h, 1), :]
        for j, span in parts:
            value = att[h, span] + row(E_BEFORE, j, h) * mm(qd[h, span], state, AB)
            att[h, span] = value
            sq_acc[span] += value * value
            in_acc[span] += g[h, span].astype(F32) * gain * value

    def keep_in(h, state):
        state_in[h] = state

    sq_acc[...] = jnp.zeros_like(sq_acc)
    in_acc[...] = jnp.zeros_like(in_acc)
    pair_copy().wait_recv()
    landed(g, heads, g_sem)
    lag = jnp.minimum(4 * forward.row, half)

    def forward_turn(i):
        at = i - lag
        ready = jnp.logical_and(at >= 0, at < half)

        @pl.when(ready)
        def _():
            forward.step(forward.led(at), keep_in)

        @pl.when(i < half)
        def _():
            intra_pair(i)

        @pl.when(ready)
        def _():
            arrive(forward.led(at))

    loop(half + lag, forward_turn)

    def forward_take(s):
        forward.take(forward.other(s), keep_in)
        arrive(forward.other(s))

    loop(half, forward_take)

    count = len(parts)
    lane = lax.broadcasted_iota(jnp.int32, (CHUNK, DH), 1)
    sums = jnp.zeros((CHUNK, DH), F32)
    for j, span in parts:
        sums = jnp.where(lane == j, jnp.sum(sq_acc[span], axis=1, keepdims=True), sums)
        sums = jnp.where(lane == count + j, jnp.sum(in_acc[span], axis=1, keepdims=True), sums)
    stat_send[...] = sums.T[0 : stat_send.shape[0]]

    def stat_copy(off):
        return remote(
            stat_send, stat_recv.at[my_head], stat_sem.at[0], stat_sem.at[1],
            "head", lax.rem(my_head + off, peers),
        )

    for off in range(1, peers):
        stat_copy(off).start()
    stat_recv[my_head] = stat_send[...]
    forward.wait_l(half)
    backward.start()
    many = stat_recv.at[0 : peers - 1]
    remote(many, many, stat_sem.at[0], stat_sem.at[1], "head", lax.rem(my_head + 1, peers)).wait_recv()
    stats = stat_recv[0]
    for i in range(1, peers):
        stats = stats + stat_recv[i]
    inverse = lax.rsqrt(stats[0:count] / width + EPSILON)
    center = stats[count : 2 * count] * inverse / width
    terms = three_terms(jnp.concatenate([inverse, center], axis=0))
    scales = jnp.concatenate(terms + [jnp.zeros((DH - 6 * count, DH), F32)], axis=0).T.astype(BF16)
    r = lax.broadcasted_iota(jnp.int32, (DH, 2 * DH), 0)
    base = jnp.where(lax.broadcasted_iota(jnp.int32, (DH, 2 * DH), 1) < DH, r, r - count)
    for j, span in parts:
        hit = (base == j) | (base == 2 * count + j) | (base == 4 * count + j)
        wide = mm(scales, jnp.where(hit, 1.0, 0.0).astype(BF16), AB)
        inv_b[span] = wide[:, :DH]
        cen_b[span] = wide[:, DH:]

    def normalize(h):
        gain = gain_ref[pl.ds(h, 1), :]
        gain_part = jnp.zeros((8, DH), F32)
        state = None
        for j, span in reversed(parts):
            scale = inv_b[span]
            normed = att[h, span] * scale
            obuf[h, span] = (normed * gain).astype(BF16)
            cotangent = g[h, span].astype(F32)
            gain_part = gain_part + jnp.sum((cotangent * normed).reshape(CHUNK // 8, 8, DH), axis=0)
            grad = (scale * (cotangent * gain - normed * cen_b[span])).astype(BF16)
            ga[h, span] = grad
            part = row(E_MID, j, h) * mm(qd[h, span], grad, ATB)
            if j < final:
                ts[h, j] = (row(E_MID, j, h) * state).astype(BF16)
            state = part if j == final else row(E_TOTAL, j, h) * state + part
        lsend[h] = state
        gain_send[pl.ds(h, 1), :] = jnp.sum(gain_part, axis=0, keepdims=True)

    def gradients(h):
        incoming = state_in[h]
        pick = jnp.concatenate([selector(columns, heads, h, 0), selector(columns, heads, h, 3)], axis=1)
        grad_weights, inter, scale = {}, {}, {}
        for j, span in parts:
            before = row(E_BEFORE, j, h) * incoming
            if j:
                before = before + qs[h, j].astype(F32)
            both = mm(ga[h, span], jnp.concatenate([v[h, span], before.astype(BF16)], axis=0), ABT)
            grad_weights[j], inter[j] = causal(both[:, :CHUNK]), both[:, CHUNK:]
        for j, span in parts:
            scale[j] = mm(columns[span], pick, AB)
            g[h, span] = (scale[j][:, DH:] * v[h, span].astype(F32)).astype(BF16)
        for j, span in parts:
            grad_q = mm(grad_weights[j], kd[h, span], AB) + inter[j]
            k[h, span] = (scale[j][:, :DH] * grad_q).astype(BF16)
        for j, span in parts:
            left, right = grad_weights[j].T, qd[h, span]
            if j < final:
                left = jnp.concatenate([left, v[h, span]], axis=1)
                right = jnp.concatenate([right, ts[h, j].T], axis=0)
            att[h, span] = scale[j][:, DH:] * mm(left, right, AB)
        for j, span in parts:
            left, right = wt[h, span], ga[h, span]
            if j < final:
                left = jnp.concatenate([left, kd[h, span]], axis=1)
                right = jnp.concatenate([right, ts[h, j]], axis=0)
            q[h, span] = mm(left, right, AB).astype(BF16)

    def keep_out(h, state):
        r_out[h] = state.astype(BF16)

    def gain_copy(off):
        return remote(
            gain_send, gain_recv.at[me], gain_sem.at[0], gain_sem.at[1], "seq", lax.rem(me + off, n),
        )

    def normalize_pair(i):
        normalize(2 * i)
        normalize(2 * i + 1)
        backward.copy_l(backward.other(i)).start()

    loop(half, normalize_pair)
    for off in range(1, n):
        gain_copy(off).start()
    back_lag = jnp.maximum(3 * backward.row - 1, 0)

    def backward_turn(i):
        at = i - back_lag

        @pl.when(jnp.logical_and(at >= 0, at < half))
        def _():
            backward.step(backward.led(at), keep_out)

        @pl.when(i < half)
        def _():
            loop(2, lambda o: gradients(2 * i + o))

    loop(half + back_lag, backward_turn)

    def backward_take(s):
        backward.take(backward.other(s), keep_out)

    loop(half, backward_take)

    gain_recv[me] = gain_send[...]
    many_gains = gain_recv.at[0 : n - 1]
    remote(many_gains, many_gains, gain_sem.at[0], gain_sem.at[1], "seq", forward.partner).wait_recv()
    gain_total = gain_recv[0]
    for i in range(1, n):
        gain_total = gain_total + gain_recv[i]
    gg_out[...] = gain_total

    pair_copy().wait_send()
    forward.wait_xz(half)
    backward.wait_l(half)
    backward.wait_xz(half)
    remote(many, many, stat_sem.at[0], stat_sem.at[1], "head", lax.rem(my_head + 1, peers)).wait_send()
    remote(many_gains, many_gains, gain_sem.at[0], gain_sem.at[1], "seq", forward.partner).wait_send()


def last_kernel(
    gv, gq, kd, vk, gk, out, after, rows, gg,
    out_hbm, gq_hbm, gk_hbm, gv_hbm, gg_hbm, k_stage, v_stage, store_sem,
):
    heads, tokens, _ = kd.shape

    def store(i, vmem, hbm, h):
        where = pl.ds(pl.multiple_of(h * DH, DH), DH)
        pltpu.make_async_copy(vmem.at[h], hbm.at[:, where], store_sem.at[i]).start()

    gains = pltpu.make_async_copy(gg, gg_hbm, store_sem.at[4])
    gains.start()

    def final_terms(h):
        state = after[h]
        for j, span in enumerate(spans(tokens)):
            decay = rows[E_AFTER, j, pl.ds(h, 1), :]
            k_stage[h, span] = (gk[h, span] + decay * mm(vk[h, span], state, ABT)).astype(BF16)
            v_stage[h, span] = (gv[h, span].astype(F32) + decay * mm(kd[h, span], state, AB)).astype(BF16)

    def two(p):
        for h in (2 * p, 2 * p + 1):
            store(0, out, out_hbm, h)
            store(1, gq, gq_hbm, h)
        for h in (2 * p, 2 * p + 1):
            final_terms(h)
        for h in (2 * p, 2 * p + 1):
            store(2, k_stage, gk_hbm, h)
            store(3, v_stage, gv_hbm, h)

    loop(heads // 2, two)
    for i in range(4):
        pltpu.make_async_copy(k_stage, k_stage, store_sem.at[i]).wait()
    gains.wait()


def on_device(n, peers, queries, key_rows, value_rows, log_decay, norm_gain, grad_out):
    tokens, width = queries.shape
    heads = width // DH
    chunks = tokens // CHUNK
    depth = -(-6 * heads // DH) * DH
    gain = norm_gain.reshape(heads, DH)
    anywhere = pl.BlockSpec(memory_space=pl.ANY)
    vmem = pl.BlockSpec(memory_space=pltpu.VMEM)
    rows = jax.ShapeDtypeStruct((tokens, width), BF16)
    gains = jax.ShapeDtypeStruct((heads, DH), F32)
    per_head = lambda *shape, dtype=F32: pltpu.VMEM((heads, *shape), dtype)
    dma = pltpu.SemaphoreType.DMA
    by_head = lambda dtype: pltpu.VMEM((heads, tokens, DH), dtype)
    states = pltpu.VMEM((heads, chunks, DH, DH), BF16)
    flat = pltpu.VMEM((tokens, DH), F32)
    stat_rows = -(-2 * chunks // 8) * 8
    q, k, kd, g, att, out, after, table, grad_gain = pl.pallas_call(
        functools.partial(main_kernel, n, peers),
        out_shape=(
            by_head(BF16), by_head(BF16), by_head(BF16), by_head(BF16), by_head(F32), by_head(BF16),
            pltpu.VMEM((heads, DH, DH), BF16),
            pltpu.VMEM((4, chunks, heads, DH), F32), pltpu.VMEM((heads, DH), F32),
        ),
        in_specs=[anywhere] * 4 + [vmem] * 2,
        out_specs=(vmem,) * 9,
        scratch_shapes=[
            *[by_head(BF16)] * 4, states, states, pltpu.VMEM((tokens, depth), BF16),
            per_head(DH, DH), flat, flat, flat, flat,
            pltpu.VMEM((heads, DH), F32), pltpu.VMEM((heads, DH), F32),
            pltpu.VMEM((stat_rows, DH), F32), pltpu.VMEM((peers, stat_rows, DH), F32),
            pltpu.VMEM((heads, DH), F32), pltpu.VMEM((n, heads, DH), F32),
            *[per_head(DH, DH)] * 6,
            dma((2, heads // 2)), dma, dma((3, heads)), dma((2, 3)), dma((2,)), dma((2,)), dma((2,)),
        ],
        compiler_params=pltpu.CompilerParams(
            collective_id=0, has_side_effects=True, vmem_limit_bytes=36 * 1024 * 1024
        ),
        name="forward_chain",
    )(queries, key_rows, value_rows, grad_out, log_decay, gain)
    out, grad_q, grad_k, grad_v, grad_gain = pl.pallas_call(
        last_kernel,
        out_shape=(rows,) * 4 + (gains,),
        in_specs=[vmem] * 9,
        out_specs=(anywhere,) * 5,
        scratch_shapes=[by_head(BF16), by_head(BF16), dma((5,))],
        compiler_params=pltpu.CompilerParams(vmem_limit_bytes=16 * 1024 * 1024),
        name="last_terms",
    )(q, k, kd, g, att, out, after, table, grad_gain)
    return out, grad_q, grad_k, grad_v, grad_gain.reshape(width)


def solution(mesh):
    in_specs = (
        P("seq", "head"),
        P("seq", "head"),
        P("seq", "head"),
        P("head", "seq"),
        P("head"),
        P("seq", "head"),
    )
    out_specs = (P("seq", "head"), P("seq", "head"), P("seq", "head"), P("seq", "head"), P("head"))
    return jax.shard_map(
        functools.partial(on_device, mesh.shape["seq"], mesh.shape["head"]),
        mesh=mesh, in_specs=in_specs, out_specs=out_specs, check_vma=False,
    )
```

```python
import functools

import jax
import jax.numpy as jnp
from jax import lax
from jax.experimental import pallas as pl
from jax.experimental.pallas import tpu as pltpu
from jax.sharding import PartitionSpec as P

DH = 128
EPSILON = 1e-06
CHUNK = 128
F32 = jnp.float32
BF16 = jnp.bfloat16
MESH = pl.DeviceIdType.MESH
HIGHEST = lax.Precision.HIGHEST

AB = ((1,), (0,))
ABT = ((1,), (1,))
ATB = ((0,), (0,))
E_MID, E_TOTAL, E_BEFORE, E_AFTER = range(4)
PIECES = (slice(0, DH // 2), slice(DH // 2, DH))


def mm(left, right, dims):
    return lax.dot_general(left, right, (dims, ((), ())), preferred_element_type=F32)


def exact(left, right, dims):
    return lax.dot_general(left, right, (dims, ((), ())), precision=HIGHEST, preferred_element_type=F32)


def remote(src, dst, send, recv, axis, target):
    return pltpu.make_async_remote_copy(
        src_ref=src, dst_ref=dst, send_sem=send, recv_sem=recv,
        device_id={axis: target}, device_id_type=MESH,
    )


def loop(count, body):
    lax.fori_loop(0, count, lambda i, c: (body(i), c)[1], 0)


def spans(tokens):
    return [slice(j * CHUNK, (j + 1) * CHUNK) for j in range(tokens // CHUNK)]


def causal(x):
    t = lax.broadcasted_iota(jnp.int32, x.shape, 0)
    s = lax.broadcasted_iota(jnp.int32, x.shape, 1)
    return jnp.where(t >= s, x, 0.0).astype(BF16)


def three_terms(x):
    high = x.astype(BF16).astype(F32)
    middle = (x - high).astype(BF16).astype(F32)
    return [high, middle, x - high - middle]


def decay_tables(ld, columns, rows, whole):
    heads, tokens = ld.shape
    below = lax.broadcasted_iota(jnp.int32, (CHUNK, CHUNK), 0)
    right = lax.broadcasted_iota(jnp.int32, (CHUNK, CHUNK), 1)
    tri = (below <= right).astype(F32).astype(BF16)
    parts = spans(tokens)
    stacked = jnp.concatenate([ld[:, span] for span in parts], axis=0)
    left = jnp.concatenate([x.astype(BF16) for x in three_terms(stacked)], axis=1)
    cum = mm(left, jnp.concatenate([tri] * 3, axis=0), AB)
    total = jnp.broadcast_to(cum[:, CHUNK - 1 : CHUNK], cum.shape)
    middle = 0.5 * total
    terms = three_terms(jnp.exp(cum - middle)) + three_terms(jnp.exp(middle - cum))
    exp_middle, exp_total = jnp.exp(middle), jnp.exp(total)
    rest = columns.shape[1] - 6 * heads
    totals = []
    for j, span in enumerate(parts):
        own = slice(j * heads, (j + 1) * heads)
        stack = [x[own] for x in terms]
        if rest:
            stack.append(jnp.zeros((rest, CHUNK), F32))
        columns[span] = jnp.concatenate(stack, axis=0).T.astype(BF16)
        rows[E_MID, j] = exp_middle[own]
        rows[E_TOTAL, j] = exp_total[own]
        totals.append(total[own])
    count = len(totals)
    run = jnp.zeros((heads, DH), F32)
    for j in range(count):
        rows[E_BEFORE, j] = jnp.exp(run + 0.5 * totals[j])
        run = run + totals[j]
    whole[...] = jnp.exp(run)
    run = jnp.zeros((heads, DH), F32)
    for j in reversed(range(count)):
        rows[E_AFTER, j] = jnp.exp(run + 0.5 * totals[j])
        run = run + totals[j]


def selector(columns, heads, h, first):
    r = lax.broadcasted_iota(jnp.int32, (columns.shape[1], DH), 0) - h - first * heads
    return jnp.where((r == 0) | (r == heads) | (r == 2 * heads), 1.0, 0.0).astype(BF16)


class Chain:
    def __init__(self, n, reverse, whole, partner_whole, bufs, recv_sems, x_sems, send_sems):
        (self.lsend, self.lrecv, self.zsend, self.zrecv, self.xsend, self.xrecv) = bufs
        self.recv_sems, self.x_sems, self.send_sems = recv_sems, x_sems, send_sems
        self.whole, self.partner_whole = whole, partner_whole
        me = lax.axis_index("seq")
        self.partner = me + 1 - 2 * lax.rem(me, 2)
        place = n - 1 - me if reverse else me
        self.later = lax.rem(place, 2)
        self.row = place // 2
        self.first = self.row == 0
        self.last = self.row == n // 2 - 1
        step = -2 if reverse else 2
        self.next = lax.rem(me + step + n, n)

    def led(self, s):
        return 2 * s + 1 - self.later

    def other(self, s):
        return 2 * s + self.later

    def copy(self, kind, src, dst, s, i, target):
        return remote(src, dst, self.send_sems.at[2 * kind], self.recv_sems.at[kind, s, i], "seq", target)

    def copy_l(self, s, i):
        src = self.lsend.at[self.other(s), PIECES[i]]
        return self.copy(0, src, self.lrecv.at[s, PIECES[i]], s, i, self.partner)

    def copy_x(self, s):
        return remote(self.xsend.at[s], self.xrecv.at[s], self.send_sems.at[1], self.x_sems.at[s], "seq", self.partner)

    def copy_z(self, s, i):
        return self.copy(1, self.zsend.at[s, PIECES[i]], self.zrecv.at[s, PIECES[i]], s, i, self.next)

    def start(self):
        @pl.when(self.first)
        def _():
            self.zrecv[...] = jnp.zeros_like(self.zrecv)

    def give(self, s):
        for i in range(len(PIECES)):
            self.copy_l(s, i).start()

    def step(self, s, take):
        h = self.led(s)
        own, theirs = self.whole[pl.ds(h, 1), :], self.partner_whole[pl.ds(h, 1), :]
        for i, piece in enumerate(PIECES):
            @pl.when(jnp.logical_not(self.first))
            def _():
                self.copy_z(s, i).wait_recv()

            self.copy_l(s, i).wait_recv()
            state, mine, other = self.zrecv[s, piece], self.lsend[h, piece], self.lrecv[s, piece]

            @pl.when(self.later == 1)
            def _():
                mid = theirs * state + other
                self.zsend[s, piece] = own * mid + mine
                self.xsend[s, piece] = state
                take(h, piece, mid)

            @pl.when(self.later == 0)
            def _():
                mid = own * state + mine
                self.zsend[s, piece] = theirs * mid + other
                self.xsend[s, piece] = mid
                take(h, piece, state)

            @pl.when(jnp.logical_not(self.last))
            def _():
                self.copy_z(s, i).start()

        self.copy_x(s).start()

    def take(self, s, take):
        self.copy_x(s).wait_recv()
        take(self.other(s), slice(0, DH), self.xrecv[s])

    def sent(self):
        half = self.xsend.shape[0]
        mine = self.lsend.at[0:half]
        self.copy(0, mine, self.lrecv, 0, 0, self.partner).wait_send()
        remote(self.xsend, self.xrecv, self.send_sems.at[1], self.x_sems.at[0], "seq", self.partner).wait_send()

        @pl.when(jnp.logical_not(self.last))
        def _():
            self.copy(1, self.zsend, self.zrecv, 0, 0, self.next).wait_send()


def main_kernel(
    n, peers,
    q_hbm, k_hbm, v_hbm, g_hbm, ld_hbm, gain_hbm,
    q, k, kd, g, att, obuf, r_out, rows, gg_out,
    v, qd, ga, wt, qs, ts, columns, ld, gain_ref, state_in, sq_acc, in_acc, inv_b, cen_b,
    whole, partner_whole,
    stat_send, stat_recv, gain_send, gain_recv,
    lsend, lrecv, zsend, zrecv, xsend, xrecv,
    once_sem, recv_sems, x_sems, send_sems, pair_sem, stat_sem, gain_sem, tokens_sem,
):
    heads, tokens, _ = q.shape
    half = heads // 2
    parts = list(enumerate(spans(tokens)))
    final = len(parts) - 1
    me = lax.axis_index("seq")
    my_head = lax.axis_index("head")
    width = heads * DH * peers

    def load(hbm, vmem, h, sem):
        where = pl.ds(pl.multiple_of(h * DH, DH), DH)
        pltpu.make_async_copy(hbm.at[:, where], vmem.at[h], sem).start()

    def landed(vmem, count, sem):
        pltpu.make_async_copy(vmem.at[0:count], vmem.at[0:count], sem).wait()

    def landed_twice(count, sem):
        pltpu.make_async_copy(att.at[0:count], att.at[0:count], sem).wait()

    def load_kv(p, sem):
        for h in (2 * p, 2 * p + 1):
            load(k_hbm, k, h, sem)
            load(v_hbm, v, h, sem)

    def load_q(p):
        for h in (2 * p, 2 * p + 1):
            load(q_hbm, q, h, once_sem.at[3])

    def load_g(p):
        for h in (2 * p, 2 * p + 1):
            load(g_hbm, g, h, once_sem.at[0])

    ld_copy = pltpu.make_async_copy(ld_hbm, ld, once_sem.at[1])
    gain_in = pltpu.make_async_copy(gain_hbm, gain_ref, once_sem.at[2])
    ld_copy.start()
    load_kv(0, once_sem.at[4])
    loop(half - 1, lambda p: load_kv(p + 1, once_sem.at[5]))
    gain_in.start()
    barrier = pltpu.get_barrier_semaphore()
    at_start, at_end = me < 2, me >= n - 2

    def signal(semaphore, axis, target):
        pl.semaphore_signal(semaphore, inc=1, device_id={axis: target}, device_id_type=MESH)

    signal(barrier, "seq", me + 1 - 2 * lax.rem(me, 2))
    for off in range(1, peers):
        signal(barrier, "head", lax.rem(my_head + off, peers))
    pl.when(jnp.logical_not(at_start))(lambda: signal(barrier, "seq", lax.rem(me + n - 2, n)))
    pl.when(jnp.logical_not(at_end))(lambda: signal(barrier, "seq", lax.rem(me + 2, n)))
    loop(half, load_q)
    loop(half, load_g)
    ld_copy.wait()
    decay_tables(ld, columns, rows, whole)
    bufs = (lsend, lrecv, zsend, zrecv, xsend, xrecv)
    forward = Chain(n, False, whole, partner_whole, bufs, recv_sems, x_sems, send_sems)
    backward = Chain(n, True, whole, partner_whole, bufs, recv_sems, x_sems, send_sems)
    forward.start()

    def row(kind, j, h):
        return rows[kind, j, pl.ds(h, 1), :]

    def local_states(group):
        keys = {}
        for i, h in enumerate(group):
            pick = selector(columns, heads, h, 3)
            for j, span in parts:
                keys[i, j] = (k[h, span].astype(F32) * mm(columns[span], pick, AB)).astype(BF16)
                kd[h, span] = keys[i, j]
        for i, h in enumerate(group):
            state = None
            for j, span in parts:
                part = row(E_MID, j, h) * mm(keys[i, j], v[h, span], ATB)
                if j:
                    qs[h, j] = (row(E_MID, j, h) * state).astype(BF16)
                state = part if j == 0 else row(E_TOTAL, j, h) * state + part
            lsend[h] = state

    def pair_copy():
        return remote(whole, partner_whole, pair_sem.at[0], pair_sem.at[1], "seq", forward.partner)

    landed(k, 4, once_sem.at[4])
    local_states([forward.other(0)])
    neighbours = peers + jnp.where(at_start, 0, 1) + jnp.where(at_end, 0, 1)
    pl.semaphore_wait(barrier, neighbours)
    forward.give(0)
    pair_copy().start()

    def pass_up():
        pl.when(jnp.logical_not(at_end))(lambda: signal(tokens_sem.at[0], "seq", lax.rem(me + 2, n)))

    def pass_down():
        pl.when(jnp.logical_not(at_start))(lambda: signal(tokens_sem.at[1], "seq", lax.rem(me + n - 2, n)))

    pl.when(at_start)(pass_up)
    pl.when(at_end)(pass_down)
    local_states([forward.led(0)])

    def local_rest(i):
        local_states([2 * i + 2, 2 * i + 3])
        forward.give(i + 1)

    landed_twice(heads - 2, once_sem.at[5])
    loop(half - 1, local_rest)

    def intra_pair(p):
        queries, weights = {}, {}
        both = [(i, j, 2 * p + i, span) for i in (0, 1) for j, span in parts]
        picks = [selector(columns, heads, 2 * p + i, 0) for i in (0, 1)]
        for i, j, h, span in both:
            queries[i, j] = (q[h, span].astype(F32) * mm(columns[span], picks[i], AB)).astype(BF16)
            qd[h, span] = queries[i, j]
        for i, j, h, span in both:
            weights[i, j] = causal(mm(queries[i, j], kd[h, span], ABT))
            wt[h, span] = weights[i, j].T
        for i, j, h, span in both:
            if j:
                left = jnp.concatenate([weights[i, j], queries[i, j]], axis=1)
                right = jnp.concatenate([v[h, span], qs[h, j]], axis=0)
                att[h, span] = mm(left, right, AB)
            else:
                att[h, span] = mm(weights[i, j], v[h, span], AB)

    def arrive(h):
        state = state_in[h].astype(BF16)
        gain = gain_ref[pl.ds(h, 1), :]
        for j, span in parts:
            value = att[h, span] + row(E_BEFORE, j, h) * mm(qd[h, span], state, AB)
            att[h, span] = value
            sq_acc[span] += value * value
            in_acc[span] += g[h, span].astype(F32) * gain * value

    def keep_in(h, piece, state):
        state_in[h, piece] = state

    sq_acc[...] = jnp.zeros_like(sq_acc)
    in_acc[...] = jnp.zeros_like(in_acc)
    pair_copy().wait_recv()
    gain_in.wait()
    landed(q, heads, once_sem.at[3])
    landed(g, heads, once_sem.at[0])
    lag = jnp.minimum(4 * forward.row, half)

    def forward_turn(i):
        at = i - lag
        ready = jnp.logical_and(at >= 0, at < half)

        @pl.when(ready)
        def _():
            forward.step(at, keep_in)

        @pl.when(i < half)
        def _():
            intra_pair(i)

        @pl.when(ready)
        def _():
            arrive(forward.led(at))

    loop(half + lag, forward_turn)

    def forward_take(s):
        forward.take(s, keep_in)
        arrive(forward.other(s))

    loop(half, forward_take)

    count = len(parts)
    lane = lax.broadcasted_iota(jnp.int32, (CHUNK, DH), 1)
    sums = jnp.zeros((CHUNK, DH), F32)
    for j, span in parts:
        sums = jnp.where(lane == j, jnp.sum(sq_acc[span], axis=1, keepdims=True), sums)
        sums = jnp.where(lane == count + j, jnp.sum(in_acc[span], axis=1, keepdims=True), sums)
    stat_send[...] = sums.T[0 : stat_send.shape[0]]

    def stat_copy(off):
        return remote(
            stat_send, stat_recv.at[my_head], stat_sem.at[0], stat_sem.at[1],
            "head", lax.rem(my_head + off, peers),
        )

    for off in range(1, peers):
        stat_copy(off).start()
    stat_recv[my_head] = stat_send[...]

    @pl.when(jnp.logical_not(at_start))
    def _():
        pl.semaphore_wait(tokens_sem.at[0], 1)
        pass_up()

    @pl.when(jnp.logical_not(at_end))
    def _():
        pl.semaphore_wait(tokens_sem.at[1], 1)
        pass_down()

    forward.sent()
    backward.start()
    many = stat_recv.at[0 : peers - 1]
    remote(many, many, stat_sem.at[0], stat_sem.at[1], "head", lax.rem(my_head + 1, peers)).wait_recv()
    stats = stat_recv[0]
    for i in range(1, peers):
        stats = stats + stat_recv[i]
    inverse = lax.rsqrt(stats[0:count] / width + EPSILON)
    center = stats[count : 2 * count] * inverse / width
    terms = three_terms(jnp.concatenate([inverse, center], axis=0))
    scales = jnp.concatenate(terms + [jnp.zeros((DH - 6 * count, DH), F32)], axis=0).T.astype(BF16)
    r = lax.broadcasted_iota(jnp.int32, (DH, 2 * DH), 0)
    base = jnp.where(lax.broadcasted_iota(jnp.int32, (DH, 2 * DH), 1) < DH, r, r - count)
    for j, span in parts:
        hit = (base == j) | (base == 2 * count + j) | (base == 4 * count + j)
        wide = mm(scales, jnp.where(hit, 1.0, 0.0).astype(BF16), AB)
        inv_b[span] = wide[:, :DH]
        cen_b[span] = wide[:, DH:]

    def normalize(h):
        gain = gain_ref[pl.ds(h, 1), :]
        gain_part = jnp.zeros((8, DH), F32)
        state = None
        for j, span in reversed(parts):
            scale = inv_b[span]
            normed = att[h, span] * scale
            obuf[h, span] = (normed * gain).astype(BF16)
            cotangent = g[h, span].astype(F32)
            gain_part = gain_part + jnp.sum((cotangent * normed).reshape(CHUNK // 8, 8, DH), axis=0)
            grad = (scale * (cotangent * gain - normed * cen_b[span])).astype(BF16)
            ga[h, span] = grad
            part = row(E_MID, j, h) * mm(qd[h, span], grad, ATB)
            if j < final:
                ts[h, j] = (row(E_MID, j, h) * state).astype(BF16)
            state = part if j == final else row(E_TOTAL, j, h) * state + part
        lsend[h] = state
        gain_send[pl.ds(h, 1), :] = jnp.sum(gain_part, axis=0, keepdims=True)

    def gradients(h):
        incoming = state_in[h]
        pick = jnp.concatenate([selector(columns, heads, h, 0), selector(columns, heads, h, 3)], axis=1)
        grad_weights, inter, scale = {}, {}, {}
        for j, span in parts:
            before = row(E_BEFORE, j, h) * incoming
            if j:
                before = before + qs[h, j].astype(F32)
            both = mm(ga[h, span], jnp.concatenate([v[h, span], before.astype(BF16)], axis=0), ABT)
            grad_weights[j], inter[j] = causal(both[:, :CHUNK]), both[:, CHUNK:]
        for j, span in parts:
            scale[j] = mm(columns[span], pick, AB)
            g[h, span] = (scale[j][:, DH:] * v[h, span].astype(F32)).astype(BF16)
        for j, span in parts:
            grad_q = mm(grad_weights[j], kd[h, span], AB) + inter[j]
            k[h, span] = (scale[j][:, :DH] * grad_q).astype(BF16)
        for j, span in parts:
            left, right = grad_weights[j].T, qd[h, span]
            if j < final:
                left = jnp.concatenate([left, v[h, span]], axis=1)
                right = jnp.concatenate([right, ts[h, j].T], axis=0)
            att[h, span] = scale[j][:, DH:] * mm(left, right, AB)
        for j, span in parts:
            left, right = wt[h, span], ga[h, span]
            if j < final:
                left = jnp.concatenate([left, kd[h, span]], axis=1)
                right = jnp.concatenate([right, ts[h, j]], axis=0)
            q[h, span] = mm(left, right, AB).astype(BF16)

    def keep_out(h, piece, state):
        r_out[h, piece] = state.astype(BF16)

    def gain_copy(off):
        return remote(
            gain_send, gain_recv.at[me], gain_sem.at[0], gain_sem.at[1], "seq", lax.rem(me + off, n),
        )

    def normalize_pair(i):
        normalize(2 * i + 2)
        normalize(2 * i + 3)
        backward.give(i + 1)

    normalize(backward.other(0))
    backward.give(0)
    normalize(backward.led(0))
    loop(half - 1, normalize_pair)
    for off in range(1, n):
        gain_copy(off).start()
    back_lag = jnp.minimum(6 * backward.row, heads)

    def backward_turn(i):
        at = i - back_lag

        @pl.when(jnp.logical_and(at >= 0, at < half))
        def _():
            backward.step(at, keep_out)

        @pl.when(i < heads)
        def _():
            gradients(i)

    loop(jnp.maximum(heads, half + back_lag), backward_turn)

    gain_recv[me] = gain_send[...]
    many_gains = gain_recv.at[0 : n - 1]
    remote(many_gains, many_gains, gain_sem.at[0], gain_sem.at[1], "seq", forward.partner).wait_recv()
    gain_total = gain_recv[0]
    for i in range(1, n):
        gain_total = gain_total + gain_recv[i]
    gg_out[...] = gain_total

    def backward_take(s):
        backward.take(s, keep_out)

    loop(half, backward_take)
    pair_copy().wait_send()
    backward.sent()
    remote(many, many, stat_sem.at[0], stat_sem.at[1], "head", lax.rem(my_head + 1, peers)).wait_send()
    remote(many_gains, many_gains, gain_sem.at[0], gain_sem.at[1], "seq", forward.partner).wait_send()


def last_kernel(
    gv, gq, kd, vk, gk, out, after, rows, gg,
    out_hbm, gq_hbm, gk_hbm, gv_hbm, gg_hbm, k_stage, v_stage, store_sem,
):
    heads, tokens, _ = kd.shape

    def store(i, vmem, hbm, h):
        where = pl.ds(pl.multiple_of(h * DH, DH), DH)
        pltpu.make_async_copy(vmem.at[h], hbm.at[:, where], store_sem.at[i]).start()

    gains = pltpu.make_async_copy(gg, gg_hbm, store_sem.at[4])
    gains.start()

    def final_terms(h):
        state = after[h]
        for j, span in enumerate(spans(tokens)):
            decay = rows[E_AFTER, j, pl.ds(h, 1), :]
            k_stage[h, span] = (gk[h, span] + decay * mm(vk[h, span], state, ABT)).astype(BF16)
            v_stage[h, span] = (gv[h, span].astype(F32) + decay * mm(kd[h, span], state, AB)).astype(BF16)

    def two(p):
        for h in (2 * p, 2 * p + 1):
            store(0, out, out_hbm, h)
            store(1, gq, gq_hbm, h)
        for h in (2 * p, 2 * p + 1):
            final_terms(h)
        for h in (2 * p, 2 * p + 1):
            store(2, k_stage, gk_hbm, h)
            store(3, v_stage, gv_hbm, h)

    loop(heads // 2, two)
    for i in range(4):
        pltpu.make_async_copy(k_stage, k_stage, store_sem.at[i]).wait()
    gains.wait()


def on_device(n, peers, queries, key_rows, value_rows, log_decay, norm_gain, grad_out):
    tokens, width = queries.shape
    heads = width // DH
    chunks = tokens // CHUNK
    depth = -(-6 * heads // DH) * DH
    gain = norm_gain.reshape(heads, DH)
    anywhere = pl.BlockSpec(memory_space=pl.ANY)
    vmem = pl.BlockSpec(memory_space=pltpu.VMEM)
    rows = jax.ShapeDtypeStruct((tokens, width), BF16)
    gains = jax.ShapeDtypeStruct((heads, DH), F32)
    per_head = lambda *shape, dtype=F32: pltpu.VMEM((heads, *shape), dtype)
    dma = pltpu.SemaphoreType.DMA
    by_head = lambda dtype: pltpu.VMEM((heads, tokens, DH), dtype)
    states = pltpu.VMEM((heads, chunks, DH, DH), BF16)
    flat = pltpu.VMEM((tokens, DH), F32)
    stat_rows = -(-2 * chunks // 8) * 8
    q, k, kd, g, att, out, after, table, grad_gain = pl.pallas_call(
        functools.partial(main_kernel, n, peers),
        out_shape=(
            by_head(BF16), by_head(BF16), by_head(BF16), by_head(BF16), by_head(F32), by_head(BF16),
            pltpu.VMEM((heads, DH, DH), BF16),
            pltpu.VMEM((4, chunks, heads, DH), F32), pltpu.VMEM((heads, DH), F32),
        ),
        in_specs=[anywhere] * 6,
        out_specs=(vmem,) * 9,
        scratch_shapes=[
            *[by_head(BF16)] * 4, states, states, pltpu.VMEM((tokens, depth), BF16),
            pltpu.VMEM((heads, tokens), F32), pltpu.VMEM((heads, DH), F32),
            per_head(DH, DH), flat, flat, flat, flat,
            pltpu.VMEM((heads, DH), F32), pltpu.VMEM((heads, DH), F32),
            pltpu.VMEM((stat_rows, DH), F32), pltpu.VMEM((peers, stat_rows, DH), F32),
            pltpu.VMEM((heads, DH), F32), pltpu.VMEM((n, heads, DH), F32),
            per_head(DH, DH), *[pltpu.VMEM((heads // 2, DH, DH), F32)] * 5,
            dma((6,)), dma((2, heads // 2, len(PIECES))), dma((heads // 2,)), dma((3,)),
            dma((2,)), dma((2,)), dma((2,)), pltpu.SemaphoreType.REGULAR((2,)),
        ],
        compiler_params=pltpu.CompilerParams(
            collective_id=0, has_side_effects=True, vmem_limit_bytes=36 * 1024 * 1024
        ),
        name="forward_chain",
    )(queries, key_rows, value_rows, grad_out, log_decay, gain)
    out, grad_q, grad_k, grad_v, grad_gain = pl.pallas_call(
        last_kernel,
        out_shape=(rows,) * 4 + (gains,),
        in_specs=[vmem] * 9,
        out_specs=(anywhere,) * 5,
        scratch_shapes=[by_head(BF16), by_head(BF16), dma((5,))],
        compiler_params=pltpu.CompilerParams(vmem_limit_bytes=16 * 1024 * 1024),
        name="last_terms",
    )(q, k, kd, g, att, out, after, table, grad_gain)
    return out, grad_q, grad_k, grad_v, grad_gain.reshape(width)


def solution(mesh):
    in_specs = (
        P("seq", "head"),
        P("seq", "head"),
        P("seq", "head"),
        P("head", "seq"),
        P("head"),
        P("seq", "head"),
    )
    out_specs = (P("seq", "head"), P("seq", "head"), P("seq", "head"), P("seq", "head"), P("head"))
    return jax.shard_map(
        functools.partial(on_device, mesh.shape["seq"], mesh.shape["head"]),
        mesh=mesh, in_specs=in_specs, out_specs=out_specs, check_vma=False,
    )
```

```python
import functools

import jax
import jax.numpy as jnp
from jax import lax
from jax.experimental import pallas as pl
from jax.experimental.pallas import tpu as pltpu
from jax.sharding import PartitionSpec as P

DH = 128
EPSILON = 1e-06
CHUNK = 128
F32 = jnp.float32
BF16 = jnp.bfloat16
MESH = pl.DeviceIdType.MESH
HIGHEST = lax.Precision.HIGHEST

AB = ((1,), (0,))
ABT = ((1,), (1,))
ATB = ((0,), (0,))
E_MID, E_TOTAL, E_BEFORE, E_AFTER = range(4)
PIECES = (slice(0, DH // 2), slice(DH // 2, DH))


def mm(left, right, dims):
    return lax.dot_general(left, right, (dims, ((), ())), preferred_element_type=F32)


def exact(left, right, dims):
    return lax.dot_general(left, right, (dims, ((), ())), precision=HIGHEST, preferred_element_type=F32)


def remote(src, dst, send, recv, axis, target):
    return pltpu.make_async_remote_copy(
        src_ref=src, dst_ref=dst, send_sem=send, recv_sem=recv,
        device_id={axis: target}, device_id_type=MESH,
    )


def loop(count, body):
    lax.fori_loop(0, count, lambda i, c: (body(i), c)[1], 0)


def spans(tokens):
    return [slice(j * CHUNK, (j + 1) * CHUNK) for j in range(tokens // CHUNK)]


def causal(x):
    t = lax.broadcasted_iota(jnp.int32, x.shape, 0)
    s = lax.broadcasted_iota(jnp.int32, x.shape, 1)
    return jnp.where(t >= s, x, 0.0).astype(BF16)


def three_terms(x):
    high = x.astype(BF16).astype(F32)
    middle = (x - high).astype(BF16).astype(F32)
    return [high, middle, x - high - middle]


def decay_tables(ld, columns, rows, whole):
    heads, tokens = ld.shape
    below = lax.broadcasted_iota(jnp.int32, (CHUNK, CHUNK), 0)
    right = lax.broadcasted_iota(jnp.int32, (CHUNK, CHUNK), 1)
    tri = (below <= right).astype(F32).astype(BF16)
    parts = spans(tokens)
    stacked = jnp.concatenate([ld[:, span] for span in parts], axis=0)
    left = jnp.concatenate([x.astype(BF16) for x in three_terms(stacked)], axis=1)
    cum = mm(left, jnp.concatenate([tri] * 3, axis=0), AB)
    total = jnp.broadcast_to(cum[:, CHUNK - 1 : CHUNK], cum.shape)
    middle = 0.5 * total
    terms = three_terms(jnp.exp(cum - middle)) + three_terms(jnp.exp(middle - cum))
    exp_middle, exp_total = jnp.exp(middle), jnp.exp(total)
    rest = columns.shape[1] - 6 * heads
    totals = []
    for j, span in enumerate(parts):
        own = slice(j * heads, (j + 1) * heads)
        stack = [x[own] for x in terms]
        if rest:
            stack.append(jnp.zeros((rest, CHUNK), F32))
        columns[span] = jnp.concatenate(stack, axis=0).T.astype(BF16)
        rows[E_MID, j] = exp_middle[own]
        rows[E_TOTAL, j] = exp_total[own]
        totals.append(total[own])
    count = len(totals)
    run = jnp.zeros((heads, DH), F32)
    for j in range(count):
        rows[E_BEFORE, j] = jnp.exp(run + 0.5 * totals[j])
        run = run + totals[j]
    whole[...] = jnp.exp(run)
    run = jnp.zeros((heads, DH), F32)
    for j in reversed(range(count)):
        rows[E_AFTER, j] = jnp.exp(run + 0.5 * totals[j])
        run = run + totals[j]


def selector(columns, heads, h, first):
    r = lax.broadcasted_iota(jnp.int32, (columns.shape[1], DH), 0) - h - first * heads
    return jnp.where((r == 0) | (r == heads) | (r == 2 * heads), 1.0, 0.0).astype(BF16)


class Chain:
    def __init__(self, n, reverse, whole, partner_whole, bufs, recv_sems, x_sems, send_sems):
        (self.lsend, self.lrecv, self.zsend, self.zrecv, self.xsend, self.xrecv) = bufs
        self.recv_sems, self.x_sems, self.send_sems = recv_sems, x_sems, send_sems
        self.whole, self.partner_whole = whole, partner_whole
        me = lax.axis_index("seq")
        self.partner = me + 1 - 2 * lax.rem(me, 2)
        place = n - 1 - me if reverse else me
        self.later = lax.rem(place, 2)
        self.row = place // 2
        self.first = self.row == 0
        self.last = self.row == n // 2 - 1
        step = -2 if reverse else 2
        self.next = lax.rem(me + step + n, n)

    def led(self, s):
        return 2 * s + 1 - self.later

    def other(self, s):
        return 2 * s + self.later

    def copy(self, kind, src, dst, s, i, target):
        return remote(src, dst, self.send_sems.at[2 * kind], self.recv_sems.at[kind, s, i], "seq", target)

    def copy_l(self, s, i):
        src = self.lsend.at[self.other(s), PIECES[i]]
        return self.copy(0, src, self.lrecv.at[s, PIECES[i]], s, i, self.partner)

    def copy_x(self, s):
        return remote(self.xsend.at[s], self.xrecv.at[s], self.send_sems.at[1], self.x_sems.at[s], "seq", self.partner)

    def copy_z(self, s, i):
        return self.copy(1, self.zsend.at[s, PIECES[i]], self.zrecv.at[s, PIECES[i]], s, i, self.next)

    def start(self):
        @pl.when(self.first)
        def _():
            self.zrecv[...] = jnp.zeros_like(self.zrecv)

    def give(self, s):
        for i in range(len(PIECES)):
            self.copy_l(s, i).start()

    def step(self, s, take):
        h = self.led(s)
        own, theirs = self.whole[pl.ds(h, 1), :], self.partner_whole[pl.ds(h, 1), :]
        for i, piece in enumerate(PIECES):
            @pl.when(jnp.logical_not(self.first))
            def _():
                self.copy_z(s, i).wait_recv()

            self.copy_l(s, i).wait_recv()
            state, mine, other = self.zrecv[s, piece], self.lsend[h, piece], self.lrecv[s, piece]

            @pl.when(self.later == 1)
            def _():
                mid = theirs * state + other
                self.zsend[s, piece] = own * mid + mine
                self.xsend[s, piece] = state
                take(h, piece, mid)

            @pl.when(self.later == 0)
            def _():
                mid = own * state + mine
                self.zsend[s, piece] = theirs * mid + other
                self.xsend[s, piece] = mid
                take(h, piece, state)

            @pl.when(jnp.logical_not(self.last))
            def _():
                self.copy_z(s, i).start()

        self.copy_x(s).start()

    def take(self, s, take):
        self.copy_x(s).wait_recv()
        take(self.other(s), slice(0, DH), self.xrecv[s])

    def sent(self):
        half = self.xsend.shape[0]
        mine = self.lsend.at[0:half]
        self.copy(0, mine, self.lrecv, 0, 0, self.partner).wait_send()
        remote(self.xsend, self.xrecv, self.send_sems.at[1], self.x_sems.at[0], "seq", self.partner).wait_send()

        @pl.when(jnp.logical_not(self.last))
        def _():
            self.copy(1, self.zsend, self.zrecv, 0, 0, self.next).wait_send()


def main_kernel(
    n, peers,
    q_hbm, k_hbm, v_hbm, g_hbm, ld_hbm, gain_hbm,
    q, k, kd, g, att, obuf, r_out, rows, gg_out,
    v, qd, ga, wt, qs, ts, columns, ld, gain_ref, state_in, sq_acc, in_acc, inv_b, cen_b,
    whole, partner_whole,
    stat_send, stat_recv, gain_send, gain_pair_recv, gain_sum, gain_recv,
    lsend, lrecv, zsend, zrecv, xsend, xrecv,
    once_sem, recv_sems, x_sems, send_sems, pair_sem, stat_sem, gain_sem, tokens_sem,
):
    heads, tokens, _ = q.shape
    half = heads // 2
    parts = list(enumerate(spans(tokens)))
    final = len(parts) - 1
    me = lax.axis_index("seq")
    my_head = lax.axis_index("head")
    width = heads * DH * peers

    def load(hbm, vmem, h, sem):
        where = pl.ds(pl.multiple_of(h * DH, DH), DH)
        pltpu.make_async_copy(hbm.at[:, where], vmem.at[h], sem).start()

    def landed(vmem, count, sem):
        pltpu.make_async_copy(vmem.at[0:count], vmem.at[0:count], sem).wait()

    def landed_twice(count, sem):
        pltpu.make_async_copy(att.at[0:count], att.at[0:count], sem).wait()

    def load_kv(p, sem):
        for h in (2 * p, 2 * p + 1):
            load(k_hbm, k, h, sem)
            load(v_hbm, v, h, sem)

    def load_q(p):
        for h in (2 * p, 2 * p + 1):
            load(q_hbm, q, h, once_sem.at[3])

    def load_g(p):
        for h in (2 * p, 2 * p + 1):
            load(g_hbm, g, h, once_sem.at[0])

    ld_copy = pltpu.make_async_copy(ld_hbm, ld, once_sem.at[1])
    gain_in = pltpu.make_async_copy(gain_hbm, gain_ref, once_sem.at[2])
    ld_copy.start()
    load_kv(0, once_sem.at[4])
    loop(half - 1, lambda p: load_kv(p + 1, once_sem.at[5]))
    gain_in.start()
    barrier = pltpu.get_barrier_semaphore()
    at_start, at_end = me < 2, me >= n - 2

    def signal(semaphore, axis, target):
        pl.semaphore_signal(semaphore, inc=1, device_id={axis: target}, device_id_type=MESH)

    signal(barrier, "seq", me + 1 - 2 * lax.rem(me, 2))
    for off in range(1, peers):
        signal(barrier, "head", lax.rem(my_head + off, peers))
    pl.when(jnp.logical_not(at_start))(lambda: signal(barrier, "seq", lax.rem(me + n - 2, n)))
    pl.when(jnp.logical_not(at_end))(lambda: signal(barrier, "seq", lax.rem(me + 2, n)))
    loop(half, load_q)
    loop(half, load_g)
    ld_copy.wait()
    decay_tables(ld, columns, rows, whole)
    bufs = (lsend, lrecv, zsend, zrecv, xsend, xrecv)
    forward = Chain(n, False, whole, partner_whole, bufs, recv_sems, x_sems, send_sems)
    backward = Chain(n, True, whole, partner_whole, bufs, recv_sems, x_sems, send_sems)
    forward.start()

    def row(kind, j, h):
        return rows[kind, j, pl.ds(h, 1), :]

    def local_states(group):
        keys = {}
        for i, h in enumerate(group):
            pick = selector(columns, heads, h, 3)
            for j, span in parts:
                keys[i, j] = (k[h, span].astype(F32) * mm(columns[span], pick, AB)).astype(BF16)
                kd[h, span] = keys[i, j]
        for i, h in enumerate(group):
            state = None
            for j, span in parts:
                part = row(E_MID, j, h) * mm(keys[i, j], v[h, span], ATB)
                if j:
                    qs[h, j] = (row(E_MID, j, h) * state).astype(BF16)
                state = part if j == 0 else row(E_TOTAL, j, h) * state + part
            lsend[h] = state

    def pair_copy():
        return remote(whole, partner_whole, pair_sem.at[0], pair_sem.at[1], "seq", forward.partner)

    landed(k, 4, once_sem.at[4])
    local_states([forward.other(0)])
    neighbours = peers + jnp.where(at_start, 0, 1) + jnp.where(at_end, 0, 1)
    pl.semaphore_wait(barrier, neighbours)
    forward.give(0)
    pair_copy().start()

    def pass_up():
        pl.when(jnp.logical_not(at_end))(lambda: signal(tokens_sem.at[0], "seq", lax.rem(me + 2, n)))

    def pass_down():
        pl.when(jnp.logical_not(at_start))(lambda: signal(tokens_sem.at[1], "seq", lax.rem(me + n - 2, n)))

    pl.when(at_start)(pass_up)
    pl.when(at_end)(pass_down)
    local_states([forward.led(0)])

    def local_rest(i):
        local_states([2 * i + 2, 2 * i + 3])
        forward.give(i + 1)

    landed_twice(heads - 2, once_sem.at[5])
    loop(half - 1, local_rest)

    def intra_pair(p):
        queries, weights = {}, {}
        both = [(i, j, 2 * p + i, span) for i in (0, 1) for j, span in parts]
        picks = [selector(columns, heads, 2 * p + i, 0) for i in (0, 1)]
        for i, j, h, span in both:
            queries[i, j] = (q[h, span].astype(F32) * mm(columns[span], picks[i], AB)).astype(BF16)
            qd[h, span] = queries[i, j]
        for i, j, h, span in both:
            weights[i, j] = causal(mm(queries[i, j], kd[h, span], ABT))
            wt[h, span] = weights[i, j].T
        for i, j, h, span in both:
            if j:
                left = jnp.concatenate([weights[i, j], queries[i, j]], axis=1)
                right = jnp.concatenate([v[h, span], qs[h, j]], axis=0)
                att[h, span] = mm(left, right, AB)
            else:
                att[h, span] = mm(weights[i, j], v[h, span], AB)

    def arrive(h):
        state = state_in[h].astype(BF16)
        gain = gain_ref[pl.ds(h, 1), :]
        for j, span in parts:
            value = att[h, span] + row(E_BEFORE, j, h) * mm(qd[h, span], state, AB)
            att[h, span] = value
            sq_acc[span] += value * value
            in_acc[span] += g[h, span].astype(F32) * gain * value

    def keep_in(h, piece, state):
        state_in[h, piece] = state

    sq_acc[...] = jnp.zeros_like(sq_acc)
    in_acc[...] = jnp.zeros_like(in_acc)
    pair_copy().wait_recv()
    gain_in.wait()
    landed(q, heads, once_sem.at[3])
    landed(g, heads, once_sem.at[0])
    lag = jnp.minimum(4 * forward.row, half)

    def forward_turn(i):
        at = i - lag
        ready = jnp.logical_and(at >= 0, at < half)

        @pl.when(ready)
        def _():
            forward.step(at, keep_in)

        @pl.when(i < half)
        def _():
            intra_pair(i)

        @pl.when(ready)
        def _():
            arrive(forward.led(at))

    loop(half + lag, forward_turn)

    def forward_take(s):
        forward.take(s, keep_in)
        arrive(forward.other(s))

    loop(half, forward_take)

    count = len(parts)
    lane = lax.broadcasted_iota(jnp.int32, (CHUNK, DH), 1)
    sums = jnp.zeros((CHUNK, DH), F32)
    for j, span in parts:
        sums = jnp.where(lane == j, jnp.sum(sq_acc[span], axis=1, keepdims=True), sums)
        sums = jnp.where(lane == count + j, jnp.sum(in_acc[span], axis=1, keepdims=True), sums)
    stat_send[...] = sums.T[0 : stat_send.shape[0]]

    def stat_copy(off):
        return remote(
            stat_send, stat_recv.at[my_head], stat_sem.at[0], stat_sem.at[1],
            "head", lax.rem(my_head + off, peers),
        )

    for off in range(1, peers):
        stat_copy(off).start()
    stat_recv[my_head] = stat_send[...]

    @pl.when(jnp.logical_not(at_start))
    def _():
        pl.semaphore_wait(tokens_sem.at[0], 1)
        pass_up()

    @pl.when(jnp.logical_not(at_end))
    def _():
        pl.semaphore_wait(tokens_sem.at[1], 1)
        pass_down()

    forward.sent()
    backward.start()
    many = stat_recv.at[0 : peers - 1]
    remote(many, many, stat_sem.at[0], stat_sem.at[1], "head", lax.rem(my_head + 1, peers)).wait_recv()
    stats = stat_recv[0]
    for i in range(1, peers):
        stats = stats + stat_recv[i]
    inverse = lax.rsqrt(stats[0:count] / width + EPSILON)
    center = stats[count : 2 * count] * inverse / width
    terms = three_terms(jnp.concatenate([inverse, center], axis=0))
    scales = jnp.concatenate(terms + [jnp.zeros((DH - 6 * count, DH), F32)], axis=0).T.astype(BF16)
    r = lax.broadcasted_iota(jnp.int32, (DH, 2 * DH), 0)
    base = jnp.where(lax.broadcasted_iota(jnp.int32, (DH, 2 * DH), 1) < DH, r, r - count)
    for j, span in parts:
        hit = (base == j) | (base == 2 * count + j) | (base == 4 * count + j)
        wide = mm(scales, jnp.where(hit, 1.0, 0.0).astype(BF16), AB)
        inv_b[span] = wide[:, :DH]
        cen_b[span] = wide[:, DH:]

    def normalize(h):
        gain = gain_ref[pl.ds(h, 1), :]
        gain_part = jnp.zeros((8, DH), F32)
        state = None
        for j, span in reversed(parts):
            scale = inv_b[span]
            normed = att[h, span] * scale
            obuf[h, span] = (normed * gain).astype(BF16)
            cotangent = g[h, span].astype(F32)
            gain_part = gain_part + jnp.sum((cotangent * normed).reshape(CHUNK // 8, 8, DH), axis=0)
            grad = (scale * (cotangent * gain - normed * cen_b[span])).astype(BF16)
            ga[h, span] = grad
            part = row(E_MID, j, h) * mm(qd[h, span], grad, ATB)
            if j < final:
                ts[h, j] = (row(E_MID, j, h) * state).astype(BF16)
            state = part if j == final else row(E_TOTAL, j, h) * state + part
        lsend[h] = state
        gain_send[pl.ds(h, 1), :] = jnp.sum(gain_part, axis=0, keepdims=True)

    def gradients(h):
        incoming = state_in[h]
        pick = jnp.concatenate([selector(columns, heads, h, 0), selector(columns, heads, h, 3)], axis=1)
        grad_weights, inter, scale = {}, {}, {}
        for j, span in parts:
            before = row(E_BEFORE, j, h) * incoming
            if j:
                before = before + qs[h, j].astype(F32)
            both = mm(ga[h, span], jnp.concatenate([v[h, span], before.astype(BF16)], axis=0), ABT)
            grad_weights[j], inter[j] = causal(both[:, :CHUNK]), both[:, CHUNK:]
        for j, span in parts:
            scale[j] = mm(columns[span], pick, AB)
            g[h, span] = (scale[j][:, DH:] * v[h, span].astype(F32)).astype(BF16)
        for j, span in parts:
            grad_q = mm(grad_weights[j], kd[h, span], AB) + inter[j]
            k[h, span] = (scale[j][:, :DH] * grad_q).astype(BF16)
        for j, span in parts:
            left, right = grad_weights[j].T, qd[h, span]
            if j < final:
                left = jnp.concatenate([left, v[h, span]], axis=1)
                right = jnp.concatenate([right, ts[h, j].T], axis=0)
            att[h, span] = scale[j][:, DH:] * mm(left, right, AB)
        for j, span in parts:
            left, right = wt[h, span], ga[h, span]
            if j < final:
                left = jnp.concatenate([left, kd[h, span]], axis=1)
                right = jnp.concatenate([right, ts[h, j]], axis=0)
            q[h, span] = mm(left, right, AB).astype(BF16)

    def keep_out(h, piece, state):
        r_out[h, piece] = state.astype(BF16)

    def gain_pair():
        return remote(gain_send, gain_pair_recv, gain_sem.at[0], gain_sem.at[1], "seq", forward.partner)

    def gain_copy(target):
        return remote(gain_sum, gain_recv.at[me // 2], gain_sem.at[2], gain_sem.at[3], "seq", target)

    def send_gains(sign):
        for k in range(1, n // 2):
            target = me + 2 * k * sign

            @pl.when(jnp.logical_and(target >= 0, target < n))
            def _():
                gain_copy(lax.rem(target + n, n)).start()

    def sum_pair():
        gain_pair().wait_recv()
        gain_sum[...] = gain_send[...] + gain_pair_recv[...]
        gain_recv[me // 2] = gain_sum[...]
        send_gains(1)

    def normalize_pair(i):
        normalize(2 * i + 2)
        normalize(2 * i + 3)
        backward.give(i + 1)

    normalize(backward.other(0))
    backward.give(0)
    normalize(backward.led(0))
    loop(half - 1, normalize_pair)
    gain_pair().start()
    back_lag = jnp.minimum(6 * backward.row, heads)

    def backward_turn(i):
        at = i - back_lag

        @pl.when(jnp.logical_and(at >= 0, at < half))
        def _():
            backward.step(at, keep_out)

        @pl.when(i < heads)
        def _():
            gradients(i)

        @pl.when(i == heads - 1)
        def _():
            sum_pair()

    loop(jnp.maximum(heads, half + back_lag), backward_turn)

    send_gains(-1)
    many_gains = gain_recv.at[0 : n // 2 - 1]
    remote(many_gains, many_gains, gain_sem.at[2], gain_sem.at[3], "seq", forward.partner).wait_recv()
    gain_total = gain_recv[0]
    for i in range(1, n // 2):
        gain_total = gain_total + gain_recv[i]
    gg_out[...] = gain_total

    def backward_take(s):
        backward.take(s, keep_out)

    loop(half, backward_take)
    pair_copy().wait_send()
    backward.sent()
    remote(many, many, stat_sem.at[0], stat_sem.at[1], "head", lax.rem(my_head + 1, peers)).wait_send()
    gain_pair().wait_send()
    remote(many_gains, many_gains, gain_sem.at[2], gain_sem.at[3], "seq", forward.partner).wait_send()


def last_kernel(
    gv, gq, kd, vk, gk, out, after, rows, gg,
    out_hbm, gq_hbm, gk_hbm, gv_hbm, gg_hbm, k_stage, v_stage, store_sem,
):
    heads, tokens, _ = kd.shape

    def store(i, vmem, hbm, h):
        where = pl.ds(pl.multiple_of(h * DH, DH), DH)
        pltpu.make_async_copy(vmem.at[h], hbm.at[:, where], store_sem.at[i]).start()

    gains = pltpu.make_async_copy(gg, gg_hbm, store_sem.at[4])
    gains.start()

    def final_terms(h):
        state = after[h]
        for j, span in enumerate(spans(tokens)):
            decay = rows[E_AFTER, j, pl.ds(h, 1), :]
            k_stage[h, span] = (gk[h, span] + decay * mm(vk[h, span], state, ABT)).astype(BF16)
            v_stage[h, span] = (gv[h, span].astype(F32) + decay * mm(kd[h, span], state, AB)).astype(BF16)

    def two(p):
        for h in (2 * p, 2 * p + 1):
            store(0, out, out_hbm, h)
            store(1, gq, gq_hbm, h)
        for h in (2 * p, 2 * p + 1):
            final_terms(h)
        for h in (2 * p, 2 * p + 1):
            store(2, k_stage, gk_hbm, h)
            store(3, v_stage, gv_hbm, h)

    loop(heads // 2, two)
    for i in range(4):
        pltpu.make_async_copy(k_stage, k_stage, store_sem.at[i]).wait()
    gains.wait()


def on_device(n, peers, queries, key_rows, value_rows, log_decay, norm_gain, grad_out):
    tokens, width = queries.shape
    heads = width // DH
    chunks = tokens // CHUNK
    depth = -(-6 * heads // DH) * DH
    gain = norm_gain.reshape(heads, DH)
    anywhere = pl.BlockSpec(memory_space=pl.ANY)
    vmem = pl.BlockSpec(memory_space=pltpu.VMEM)
    rows = jax.ShapeDtypeStruct((tokens, width), BF16)
    gains = jax.ShapeDtypeStruct((heads, DH), F32)
    per_head = lambda *shape, dtype=F32: pltpu.VMEM((heads, *shape), dtype)
    dma = pltpu.SemaphoreType.DMA
    by_head = lambda dtype: pltpu.VMEM((heads, tokens, DH), dtype)
    states = pltpu.VMEM((heads, chunks, DH, DH), BF16)
    flat = pltpu.VMEM((tokens, DH), F32)
    stat_rows = -(-2 * chunks // 8) * 8
    q, k, kd, g, att, out, after, table, grad_gain = pl.pallas_call(
        functools.partial(main_kernel, n, peers),
        out_shape=(
            by_head(BF16), by_head(BF16), by_head(BF16), by_head(BF16), by_head(F32), by_head(BF16),
            pltpu.VMEM((heads, DH, DH), BF16),
            pltpu.VMEM((4, chunks, heads, DH), F32), pltpu.VMEM((heads, DH), F32),
        ),
        in_specs=[anywhere] * 6,
        out_specs=(vmem,) * 9,
        scratch_shapes=[
            *[by_head(BF16)] * 4, states, states, pltpu.VMEM((tokens, depth), BF16),
            pltpu.VMEM((heads, tokens), F32), pltpu.VMEM((heads, DH), F32),
            per_head(DH, DH), flat, flat, flat, flat,
            pltpu.VMEM((heads, DH), F32), pltpu.VMEM((heads, DH), F32),
            pltpu.VMEM((stat_rows, DH), F32), pltpu.VMEM((peers, stat_rows, DH), F32),
            *[pltpu.VMEM((heads, DH), F32)] * 3, pltpu.VMEM((n // 2, heads, DH), F32),
            per_head(DH, DH), *[pltpu.VMEM((heads // 2, DH, DH), F32)] * 5,
            dma((6,)), dma((2, heads // 2, len(PIECES))), dma((heads // 2,)), dma((3,)),
            dma((2,)), dma((2,)), dma((4,)), pltpu.SemaphoreType.REGULAR((2,)),
        ],
        compiler_params=pltpu.CompilerParams(
            collective_id=0, has_side_effects=True, vmem_limit_bytes=36 * 1024 * 1024
        ),
        name="forward_chain",
    )(queries, key_rows, value_rows, grad_out, log_decay, gain)
    out, grad_q, grad_k, grad_v, grad_gain = pl.pallas_call(
        last_kernel,
        out_shape=(rows,) * 4 + (gains,),
        in_specs=[vmem] * 9,
        out_specs=(anywhere,) * 5,
        scratch_shapes=[by_head(BF16), by_head(BF16), dma((5,))],
        compiler_params=pltpu.CompilerParams(vmem_limit_bytes=16 * 1024 * 1024),
        name="last_terms",
    )(q, k, kd, g, att, out, after, table, grad_gain)
    return out, grad_q, grad_k, grad_v, grad_gain.reshape(width)


def solution(mesh):
    in_specs = (
        P("seq", "head"),
        P("seq", "head"),
        P("seq", "head"),
        P("head", "seq"),
        P("head"),
        P("seq", "head"),
    )
    out_specs = (P("seq", "head"), P("seq", "head"), P("seq", "head"), P("seq", "head"), P("head"))
    return jax.shard_map(
        functools.partial(on_device, mesh.shape["seq"], mesh.shape["head"]),
        mesh=mesh, in_specs=in_specs, out_specs=out_specs, check_vma=False,
    )
```

```python
import functools

import jax
import jax.numpy as jnp
from jax import lax
from jax.experimental import pallas as pl
from jax.experimental.pallas import tpu as pltpu
from jax.sharding import PartitionSpec as P

DH = 128
EPSILON = 1e-06
CHUNK = 128
F32 = jnp.float32
BF16 = jnp.bfloat16
MESH = pl.DeviceIdType.MESH
HIGHEST = lax.Precision.HIGHEST

AB = ((1,), (0,))
ABT = ((1,), (1,))
ATB = ((0,), (0,))
E_MID, E_TOTAL, E_BEFORE, E_AFTER = range(4)
PIECES = (slice(0, DH // 2), slice(DH // 2, DH))


def mm(left, right, dims):
    return lax.dot_general(left, right, (dims, ((), ())), preferred_element_type=F32)


def exact(left, right, dims):
    return lax.dot_general(left, right, (dims, ((), ())), precision=HIGHEST, preferred_element_type=F32)


def remote(src, dst, send, recv, axis, target):
    return pltpu.make_async_remote_copy(
        src_ref=src, dst_ref=dst, send_sem=send, recv_sem=recv,
        device_id={axis: target}, device_id_type=MESH,
    )


def loop(count, body):
    lax.fori_loop(0, count, lambda i, c: (body(i), c)[1], 0)


def spans(tokens):
    return [slice(j * CHUNK, (j + 1) * CHUNK) for j in range(tokens // CHUNK)]


def causal(x):
    t = lax.broadcasted_iota(jnp.int32, x.shape, 0)
    s = lax.broadcasted_iota(jnp.int32, x.shape, 1)
    return jnp.where(t >= s, x, 0.0).astype(BF16)


def three_terms(x):
    high = x.astype(BF16).astype(F32)
    middle = (x - high).astype(BF16).astype(F32)
    return [high, middle, x - high - middle]


def decay_tables(ld, columns, rows, whole):
    heads, tokens = ld.shape
    below = lax.broadcasted_iota(jnp.int32, (CHUNK, CHUNK), 0)
    right = lax.broadcasted_iota(jnp.int32, (CHUNK, CHUNK), 1)
    tri = (below <= right).astype(F32).astype(BF16)
    parts = spans(tokens)
    stacked = jnp.concatenate([ld[:, span] for span in parts], axis=0)
    left = jnp.concatenate([x.astype(BF16) for x in three_terms(stacked)], axis=1)
    cum = mm(left, jnp.concatenate([tri] * 3, axis=0), AB)
    total = jnp.broadcast_to(cum[:, CHUNK - 1 : CHUNK], cum.shape)
    middle = 0.5 * total
    terms = three_terms(jnp.exp(cum - middle)) + three_terms(jnp.exp(middle - cum))
    exp_middle, exp_total = jnp.exp(middle), jnp.exp(total)
    rest = columns.shape[1] - 6 * heads
    totals = []
    for j, span in enumerate(parts):
        own = slice(j * heads, (j + 1) * heads)
        stack = [x[own] for x in terms]
        if rest:
            stack.append(jnp.zeros((rest, CHUNK), F32))
        columns[span] = jnp.concatenate(stack, axis=0).T.astype(BF16)
        rows[E_MID, j] = exp_middle[own]
        rows[E_TOTAL, j] = exp_total[own]
        totals.append(total[own])
    count = len(totals)
    run = jnp.zeros((heads, DH), F32)
    for j in range(count):
        rows[E_BEFORE, j] = jnp.exp(run + 0.5 * totals[j])
        run = run + totals[j]
    whole[...] = jnp.exp(run)
    run = jnp.zeros((heads, DH), F32)
    for j in reversed(range(count)):
        rows[E_AFTER, j] = jnp.exp(run + 0.5 * totals[j])
        run = run + totals[j]


def selector(columns, heads, h, first):
    r = lax.broadcasted_iota(jnp.int32, (columns.shape[1], DH), 0) - h - first * heads
    return jnp.where((r == 0) | (r == heads) | (r == 2 * heads), 1.0, 0.0).astype(BF16)


class Chain:
    def __init__(self, n, reverse, whole, partner_whole, bufs, recv_sems, x_sems, send_sems):
        (self.lsend, self.lrecv, self.zsend, self.zrecv, self.xsend, self.xrecv) = bufs
        self.recv_sems, self.x_sems, self.send_sems = recv_sems, x_sems, send_sems
        self.whole, self.partner_whole = whole, partner_whole
        me = lax.axis_index("seq")
        self.partner = me + 1 - 2 * lax.rem(me, 2)
        place = n - 1 - me if reverse else me
        self.later = lax.rem(place, 2)
        self.row = place // 2
        self.first = self.row == 0
        self.last = self.row == n // 2 - 1
        step = -2 if reverse else 2
        self.next = lax.rem(me + step + n, n)

    def led(self, s):
        return 2 * s + 1 - self.later

    def other(self, s):
        return 2 * s + self.later

    def copy(self, kind, src, dst, s, i, target):
        return remote(src, dst, self.send_sems.at[2 * kind], self.recv_sems.at[kind, s, i], "seq", target)

    def copy_l(self, s, i):
        src = self.lsend.at[self.other(s), PIECES[i]]
        return self.copy(0, src, self.lrecv.at[s, PIECES[i]], s, i, self.partner)

    def copy_x(self, s):
        return remote(self.xsend.at[s], self.xrecv.at[s], self.send_sems.at[1], self.x_sems.at[s], "seq", self.partner)

    def copy_z(self, s, i):
        return self.copy(1, self.zsend.at[s, PIECES[i]], self.zrecv.at[s, PIECES[i]], s, i, self.next)

    def start(self):
        @pl.when(self.first)
        def _():
            self.zrecv[...] = jnp.zeros_like(self.zrecv)

    def give(self, s):
        for i in range(len(PIECES)):
            self.copy_l(s, i).start()

    def step(self, s, take, send_x=True):
        h = self.led(s)
        own, theirs = self.whole[pl.ds(h, 1), :], self.partner_whole[pl.ds(h, 1), :]
        for i, piece in enumerate(PIECES):
            @pl.when(jnp.logical_not(self.first))
            def _():
                self.copy_z(s, i).wait_recv()

            self.copy_l(s, i).wait_recv()
            state, mine, other = self.zrecv[s, piece], self.lsend[h, piece], self.lrecv[s, piece]

            @pl.when(self.later == 1)
            def _():
                mid = theirs * state + other
                self.zsend[s, piece] = own * mid + mine
                self.xsend[s, piece] = state
                take(h, piece, mid)

            @pl.when(self.later == 0)
            def _():
                mid = own * state + mine
                self.zsend[s, piece] = theirs * mid + other
                self.xsend[s, piece] = mid
                take(h, piece, state)

            @pl.when(jnp.logical_not(self.last))
            def _():
                self.copy_z(s, i).start()

        if send_x:
            self.copy_x(s).start()

    def take(self, s, take):
        self.copy_x(s).wait_recv()
        take(self.other(s), slice(0, DH), self.xrecv[s])

    def sent(self):
        half = self.xsend.shape[0]
        mine = self.lsend.at[0:half]
        self.copy(0, mine, self.lrecv, 0, 0, self.partner).wait_send()
        remote(self.xsend, self.xrecv, self.send_sems.at[1], self.x_sems.at[0], "seq", self.partner).wait_send()

        @pl.when(jnp.logical_not(self.last))
        def _():
            self.copy(1, self.zsend, self.zrecv, 0, 0, self.next).wait_send()


def main_kernel(
    n, peers,
    q_hbm, k_hbm, v_hbm, g_hbm, ld_hbm, gain_hbm,
    q, k, kd, g, att, obuf, r_out, rows, gg_out,
    v, qd, ga, wt, qs, ts, columns, ld, gain_ref, state_in, sq_acc, in_acc, inv_b, cen_b,
    whole, partner_whole,
    stat_send, stat_recv, gain_send, gain_pair_recv, gain_sum, gain_recv,
    lsend, lrecv, zsend, zrecv, xsend, xrecv,
    once_sem, recv_sems, x_sems, send_sems, pair_sem, stat_sem, gain_sem, tokens_sem,
):
    heads, tokens, _ = q.shape
    half = heads // 2
    parts = list(enumerate(spans(tokens)))
    final = len(parts) - 1
    me = lax.axis_index("seq")
    my_head = lax.axis_index("head")
    width = heads * DH * peers

    def load(hbm, vmem, h, sem):
        where = pl.ds(pl.multiple_of(h * DH, DH), DH)
        pltpu.make_async_copy(hbm.at[:, where], vmem.at[h], sem).start()

    def landed(vmem, count, sem):
        pltpu.make_async_copy(vmem.at[0:count], vmem.at[0:count], sem).wait()

    def landed_twice(count, sem):
        pltpu.make_async_copy(att.at[0:count], att.at[0:count], sem).wait()

    def load_kv(p, sem):
        for h in (2 * p, 2 * p + 1):
            load(k_hbm, k, h, sem)
            load(v_hbm, v, h, sem)

    def load_q(p):
        for h in (2 * p, 2 * p + 1):
            load(q_hbm, q, h, once_sem.at[3])

    def load_g(p):
        for h in (2 * p, 2 * p + 1):
            load(g_hbm, g, h, once_sem.at[0])

    ld_copy = pltpu.make_async_copy(ld_hbm, ld, once_sem.at[1])
    gain_in = pltpu.make_async_copy(gain_hbm, gain_ref, once_sem.at[2])
    ld_copy.start()
    load_kv(0, once_sem.at[4])
    loop(half - 1, lambda p: load_kv(p + 1, once_sem.at[5]))
    gain_in.start()
    barrier = pltpu.get_barrier_semaphore()
    at_start, at_end = me < 2, me >= n - 2

    def signal(semaphore, axis, target):
        pl.semaphore_signal(semaphore, inc=1, device_id={axis: target}, device_id_type=MESH)

    signal(barrier, "seq", me + 1 - 2 * lax.rem(me, 2))
    for off in range(1, peers):
        signal(barrier, "head", lax.rem(my_head + off, peers))
    pl.when(jnp.logical_not(at_start))(lambda: signal(barrier, "seq", lax.rem(me + n - 2, n)))
    pl.when(jnp.logical_not(at_end))(lambda: signal(barrier, "seq", lax.rem(me + 2, n)))
    loop(half, load_q)
    loop(half, load_g)
    ld_copy.wait()
    decay_tables(ld, columns, rows, whole)
    bufs = (lsend, lrecv, zsend, zrecv, xsend, xrecv)
    forward = Chain(n, False, whole, partner_whole, bufs, recv_sems, x_sems, send_sems)
    backward = Chain(n, True, whole, partner_whole, bufs, recv_sems, x_sems, send_sems)
    forward.start()

    def row(kind, j, h):
        return rows[kind, j, pl.ds(h, 1), :]

    def local_states(group):
        keys = {}
        for i, h in enumerate(group):
            pick = selector(columns, heads, h, 3)
            for j, span in parts:
                keys[i, j] = (k[h, span].astype(F32) * mm(columns[span], pick, AB)).astype(BF16)
                kd[h, span] = keys[i, j]
        for i, h in enumerate(group):
            state = None
            for j, span in parts:
                part = row(E_MID, j, h) * mm(keys[i, j], v[h, span], ATB)
                if j:
                    qs[h, j] = (row(E_MID, j, h) * state).astype(BF16)
                state = part if j == 0 else row(E_TOTAL, j, h) * state + part
            lsend[h] = state

    def pair_copy():
        return remote(whole, partner_whole, pair_sem.at[0], pair_sem.at[1], "seq", forward.partner)

    landed(k, 4, once_sem.at[4])
    local_states([forward.other(0)])
    neighbours = peers + jnp.where(at_start, 0, 1) + jnp.where(at_end, 0, 1)
    pl.semaphore_wait(barrier, neighbours)
    forward.give(0)
    pair_copy().start()

    def pass_up():
        pl.when(jnp.logical_not(at_end))(lambda: signal(tokens_sem.at[0], "seq", lax.rem(me + 2, n)))

    def pass_down():
        pl.when(jnp.logical_not(at_start))(lambda: signal(tokens_sem.at[1], "seq", lax.rem(me + n - 2, n)))

    pl.when(at_start)(pass_up)
    pl.when(at_end)(pass_down)
    local_states([forward.led(0)])

    def keep_in(h, piece, state):
        state_in[h, piece] = state

    def local_rest(i):
        @pl.when(i == half - 2)
        def _():
            pair_copy().wait_recv()
            gain_in.wait()

        @pl.when(jnp.logical_and(i == half - 2, forward.first))
        def _():
            forward.step(0, keep_in, send_x=False)

        local_states([2 * i + 2, 2 * i + 3])
        forward.give(i + 1)

    landed_twice(heads - 2, once_sem.at[5])
    loop(half - 1, local_rest)

    def intra_pair(p):
        queries, weights = {}, {}
        both = [(i, j, 2 * p + i, span) for i in (0, 1) for j, span in parts]
        picks = [selector(columns, heads, 2 * p + i, 0) for i in (0, 1)]
        for i, j, h, span in both:
            queries[i, j] = (q[h, span].astype(F32) * mm(columns[span], picks[i], AB)).astype(BF16)
            qd[h, span] = queries[i, j]
        for i, j, h, span in both:
            weights[i, j] = causal(mm(queries[i, j], kd[h, span], ABT))
            wt[h, span] = weights[i, j].T
        for i, j, h, span in both:
            if j:
                left = jnp.concatenate([weights[i, j], queries[i, j]], axis=1)
                right = jnp.concatenate([v[h, span], qs[h, j]], axis=0)
                att[h, span] = mm(left, right, AB)
            else:
                att[h, span] = mm(weights[i, j], v[h, span], AB)

    def arrive(h):
        state = state_in[h].astype(BF16)
        gain = gain_ref[pl.ds(h, 1), :]
        for j, span in parts:
            value = att[h, span] + row(E_BEFORE, j, h) * mm(qd[h, span], state, AB)
            att[h, span] = value
            sq_acc[span] += value * value
            in_acc[span] += g[h, span].astype(F32) * gain * value


    sq_acc[...] = jnp.zeros_like(sq_acc)
    in_acc[...] = jnp.zeros_like(in_acc)
    pl.when(forward.first)(lambda: forward.copy_x(0).start())
    landed(q, heads, once_sem.at[3])
    landed(g, heads, once_sem.at[0])
    lag = jnp.minimum(3 * forward.row, half)

    def forward_turn(i):
        at = i - lag
        turn = at + jnp.where(forward.first, 1, 0)

        @pl.when(jnp.logical_and(turn >= 0, turn < half))
        def _():
            forward.step(turn, keep_in)

        @pl.when(i < half)
        def _():
            intra_pair(i)

        @pl.when(jnp.logical_and(at >= 0, at < half))
        def _():
            arrive(forward.led(at))

    loop(half + lag, forward_turn)

    def forward_take(s):
        forward.take(s, keep_in)
        arrive(forward.other(s))

    loop(half, forward_take)

    count = len(parts)
    lane = lax.broadcasted_iota(jnp.int32, (CHUNK, DH), 1)
    sums = jnp.zeros((CHUNK, DH), F32)
    for j, span in parts:
        sums = jnp.where(lane == j, jnp.sum(sq_acc[span], axis=1, keepdims=True), sums)
        sums = jnp.where(lane == count + j, jnp.sum(in_acc[span], axis=1, keepdims=True), sums)
    stat_send[...] = sums.T[0 : stat_send.shape[0]]

    def stat_copy(off):
        return remote(
            stat_send, stat_recv.at[my_head], stat_sem.at[0], stat_sem.at[1],
            "head", lax.rem(my_head + off, peers),
        )

    for off in range(1, peers):
        stat_copy(off).start()
    stat_recv[my_head] = stat_send[...]

    @pl.when(jnp.logical_not(at_start))
    def _():
        pl.semaphore_wait(tokens_sem.at[0], 1)
        pass_up()

    @pl.when(jnp.logical_not(at_end))
    def _():
        pl.semaphore_wait(tokens_sem.at[1], 1)
        pass_down()

    forward.sent()
    backward.start()
    many = stat_recv.at[0 : peers - 1]
    remote(many, many, stat_sem.at[0], stat_sem.at[1], "head", lax.rem(my_head + 1, peers)).wait_recv()
    stats = stat_recv[0]
    for i in range(1, peers):
        stats = stats + stat_recv[i]
    inverse = lax.rsqrt(stats[0:count] / width + EPSILON)
    center = stats[count : 2 * count] * inverse / width
    terms = three_terms(jnp.concatenate([inverse, center], axis=0))
    scales = jnp.concatenate(terms + [jnp.zeros((DH - 6 * count, DH), F32)], axis=0).T.astype(BF16)
    r = lax.broadcasted_iota(jnp.int32, (DH, 2 * DH), 0)
    base = jnp.where(lax.broadcasted_iota(jnp.int32, (DH, 2 * DH), 1) < DH, r, r - count)
    for j, span in parts:
        hit = (base == j) | (base == 2 * count + j) | (base == 4 * count + j)
        wide = mm(scales, jnp.where(hit, 1.0, 0.0).astype(BF16), AB)
        inv_b[span] = wide[:, :DH]
        cen_b[span] = wide[:, DH:]

    def normalize(h):
        gain = gain_ref[pl.ds(h, 1), :]
        gain_part = jnp.zeros((8, DH), F32)
        state = None
        for j, span in reversed(parts):
            scale = inv_b[span]
            normed = att[h, span] * scale
            obuf[h, span] = (normed * gain).astype(BF16)
            cotangent = g[h, span].astype(F32)
            gain_part = gain_part + jnp.sum((cotangent * normed).reshape(CHUNK // 8, 8, DH), axis=0)
            grad = (scale * (cotangent * gain - normed * cen_b[span])).astype(BF16)
            ga[h, span] = grad
            part = row(E_MID, j, h) * mm(qd[h, span], grad, ATB)
            if j < final:
                ts[h, j] = (row(E_MID, j, h) * state).astype(BF16)
            state = part if j == final else row(E_TOTAL, j, h) * state + part
        lsend[h] = state
        gain_send[pl.ds(h, 1), :] = jnp.sum(gain_part, axis=0, keepdims=True)

    def gradients(h):
        incoming = state_in[h]
        pick = jnp.concatenate([selector(columns, heads, h, 0), selector(columns, heads, h, 3)], axis=1)
        grad_weights, inter, scale = {}, {}, {}
        for j, span in parts:
            before = row(E_BEFORE, j, h) * incoming
            if j:
                before = before + qs[h, j].astype(F32)
            both = mm(ga[h, span], jnp.concatenate([v[h, span], before.astype(BF16)], axis=0), ABT)
            grad_weights[j], inter[j] = causal(both[:, :CHUNK]), both[:, CHUNK:]
        for j, span in parts:
            scale[j] = mm(columns[span], pick, AB)
            g[h, span] = (scale[j][:, DH:] * v[h, span].astype(F32)).astype(BF16)
        for j, span in parts:
            grad_q = mm(grad_weights[j], kd[h, span], AB) + inter[j]
            k[h, span] = (scale[j][:, :DH] * grad_q).astype(BF16)
        for j, span in parts:
            left, right = grad_weights[j].T, qd[h, span]
            if j < final:
                left = jnp.concatenate([left, v[h, span]], axis=1)
                right = jnp.concatenate([right, ts[h, j].T], axis=0)
            att[h, span] = scale[j][:, DH:] * mm(left, right, AB)
        for j, span in parts:
            left, right = wt[h, span], ga[h, span]
            if j < final:
                left = jnp.concatenate([left, kd[h, span]], axis=1)
                right = jnp.concatenate([right, ts[h, j]], axis=0)
            q[h, span] = mm(left, right, AB).astype(BF16)

    def keep_out(h, piece, state):
        r_out[h, piece] = state.astype(BF16)

    def gain_pair():
        return remote(gain_send, gain_pair_recv, gain_sem.at[0], gain_sem.at[1], "seq", forward.partner)

    def gain_copy(target):
        return remote(gain_sum, gain_recv.at[me // 2], gain_sem.at[2], gain_sem.at[3], "seq", target)

    def send_gains(sign):
        for k in range(1, n // 2):
            target = me + 2 * k * sign

            @pl.when(jnp.logical_and(target >= 0, target < n))
            def _():
                gain_copy(lax.rem(target + n, n)).start()

    def sum_pair():
        gain_pair().wait_recv()
        gain_sum[...] = gain_send[...] + gain_pair_recv[...]
        gain_recv[me // 2] = gain_sum[...]
        send_gains(1)

    def normalize_pair(i):
        normalize(2 * i + 2)
        normalize(2 * i + 3)
        backward.give(i + 1)

    normalize(backward.other(0))
    backward.give(0)
    normalize(backward.led(0))
    loop(half - 1, normalize_pair)
    gain_pair().start()
    back_lag = jnp.minimum(6 * backward.row, heads)

    def backward_turn(i):
        at = i - back_lag

        @pl.when(jnp.logical_and(at >= 0, at < half))
        def _():
            backward.step(at, keep_out)

        @pl.when(i < heads)
        def _():
            gradients(i)

        @pl.when(i == heads - 1)
        def _():
            sum_pair()

    loop(jnp.maximum(heads, half + back_lag), backward_turn)

    send_gains(-1)
    many_gains = gain_recv.at[0 : n // 2 - 1]
    remote(many_gains, many_gains, gain_sem.at[2], gain_sem.at[3], "seq", forward.partner).wait_recv()
    gain_total = gain_recv[0]
    for i in range(1, n // 2):
        gain_total = gain_total + gain_recv[i]
    gg_out[...] = gain_total

    def backward_take(s):
        backward.take(s, keep_out)

    loop(half, backward_take)
    pair_copy().wait_send()
    backward.sent()
    remote(many, many, stat_sem.at[0], stat_sem.at[1], "head", lax.rem(my_head + 1, peers)).wait_send()
    gain_pair().wait_send()
    remote(many_gains, many_gains, gain_sem.at[2], gain_sem.at[3], "seq", forward.partner).wait_send()


def last_kernel(
    gv, gq, kd, vk, gk, out, after, rows, gg,
    out_hbm, gq_hbm, gk_hbm, gv_hbm, gg_hbm, k_stage, v_stage, store_sem,
):
    heads, tokens, _ = kd.shape

    def store(i, vmem, hbm, h):
        where = pl.ds(pl.multiple_of(h * DH, DH), DH)
        pltpu.make_async_copy(vmem.at[h], hbm.at[:, where], store_sem.at[i]).start()

    gains = pltpu.make_async_copy(gg, gg_hbm, store_sem.at[4])
    gains.start()

    def final_terms(h):
        state = after[h]
        for j, span in enumerate(spans(tokens)):
            decay = rows[E_AFTER, j, pl.ds(h, 1), :]
            k_stage[h, span] = (gk[h, span] + decay * mm(vk[h, span], state, ABT)).astype(BF16)
            v_stage[h, span] = (gv[h, span].astype(F32) + decay * mm(kd[h, span], state, AB)).astype(BF16)

    def two(p):
        for h in (2 * p, 2 * p + 1):
            store(0, out, out_hbm, h)
            store(1, gq, gq_hbm, h)
        for h in (2 * p, 2 * p + 1):
            final_terms(h)
        for h in (2 * p, 2 * p + 1):
            store(2, k_stage, gk_hbm, h)
            store(3, v_stage, gv_hbm, h)

    loop(heads // 2, two)
    for i in range(4):
        pltpu.make_async_copy(k_stage, k_stage, store_sem.at[i]).wait()
    gains.wait()


def on_device(n, peers, queries, key_rows, value_rows, log_decay, norm_gain, grad_out):
    tokens, width = queries.shape
    heads = width // DH
    chunks = tokens // CHUNK
    depth = -(-6 * heads // DH) * DH
    gain = norm_gain.reshape(heads, DH)
    anywhere = pl.BlockSpec(memory_space=pl.ANY)
    vmem = pl.BlockSpec(memory_space=pltpu.VMEM)
    rows = jax.ShapeDtypeStruct((tokens, width), BF16)
    gains = jax.ShapeDtypeStruct((heads, DH), F32)
    per_head = lambda *shape, dtype=F32: pltpu.VMEM((heads, *shape), dtype)
    dma = pltpu.SemaphoreType.DMA
    by_head = lambda dtype: pltpu.VMEM((heads, tokens, DH), dtype)
    states = pltpu.VMEM((heads, chunks, DH, DH), BF16)
    flat = pltpu.VMEM((tokens, DH), F32)
    stat_rows = -(-2 * chunks // 8) * 8
    q, k, kd, g, att, out, after, table, grad_gain = pl.pallas_call(
        functools.partial(main_kernel, n, peers),
        out_shape=(
            by_head(BF16), by_head(BF16), by_head(BF16), by_head(BF16), by_head(F32), by_head(BF16),
            pltpu.VMEM((heads, DH, DH), BF16),
            pltpu.VMEM((4, chunks, heads, DH), F32), pltpu.VMEM((heads, DH), F32),
        ),
        in_specs=[anywhere] * 6,
        out_specs=(vmem,) * 9,
        scratch_shapes=[
            *[by_head(BF16)] * 4, states, states, pltpu.VMEM((tokens, depth), BF16),
            pltpu.VMEM((heads, tokens), F32), pltpu.VMEM((heads, DH), F32),
            per_head(DH, DH), flat, flat, flat, flat,
            pltpu.VMEM((heads, DH), F32), pltpu.VMEM((heads, DH), F32),
            pltpu.VMEM((stat_rows, DH), F32), pltpu.VMEM((peers, stat_rows, DH), F32),
            *[pltpu.VMEM((heads, DH), F32)] * 3, pltpu.VMEM((n // 2, heads, DH), F32),
            per_head(DH, DH), *[pltpu.VMEM((heads // 2, DH, DH), F32)] * 5,
            dma((6,)), dma((2, heads // 2, len(PIECES))), dma((heads // 2,)), dma((3,)),
            dma((2,)), dma((2,)), dma((4,)), pltpu.SemaphoreType.REGULAR((2,)),
        ],
        compiler_params=pltpu.CompilerParams(
            collective_id=0, has_side_effects=True, vmem_limit_bytes=36 * 1024 * 1024
        ),
        name="forward_chain",
    )(queries, key_rows, value_rows, grad_out, log_decay, gain)
    out, grad_q, grad_k, grad_v, grad_gain = pl.pallas_call(
        last_kernel,
        out_shape=(rows,) * 4 + (gains,),
        in_specs=[vmem] * 9,
        out_specs=(anywhere,) * 5,
        scratch_shapes=[by_head(BF16), by_head(BF16), dma((5,))],
        compiler_params=pltpu.CompilerParams(vmem_limit_bytes=16 * 1024 * 1024),
        name="last_terms",
    )(q, k, kd, g, att, out, after, table, grad_gain)
    return out, grad_q, grad_k, grad_v, grad_gain.reshape(width)


def solution(mesh):
    in_specs = (
        P("seq", "head"),
        P("seq", "head"),
        P("seq", "head"),
        P("head", "seq"),
        P("head"),
        P("seq", "head"),
    )
    out_specs = (P("seq", "head"), P("seq", "head"), P("seq", "head"), P("seq", "head"), P("head"))
    return jax.shard_map(
        functools.partial(on_device, mesh.shape["seq"], mesh.shape["head"]),
        mesh=mesh, in_specs=in_specs, out_specs=out_specs, check_vma=False,
    )
```
